32 devices in a mesh: data: 1 (over z), stage: 32 (over y, x, core).
Axes of the slice: x: 4, y: 4, z: 1, core: 2. Of those that a mesh axis runs over, the one named last changes fastest.
The devices are a block of a 4x4x8 slice.
Arguments:
- micro_in: bfloat16 [32, 128, 512], P('data')
- targets: bfloat16 [32, 128, 512], P('data')
- w_in: bfloat16 [32, 2, 512, 1024], P('stage')
- w_out: bfloat16 [32, 2, 1024, 512], P('stage')
Outputs:
- output 1: float32 [32, 2, 512, 1024], P(('data', 'stage'))
- output 2: float32 [32, 2, 1024, 512], P(('data', 'stage'))
- output 3: float32 [1], P('data')
All inputs are finite; a program needn't handle non-finite values.
Results may differ from the reference program's by a relative error of at most 0.00710874.
Values are sent between devices in bfloat16 or wider.
A program may use at most 768 MiB of HBM per device.

```python
import jax
import jax.numpy as jnp
from jax import lax

STAGES = 32
MICRO = 32
TOKENS = 128
D = 512
FF = 1024


def setup_inputs(seed: int = 0, part: int = 0) -> dict:
    part_key = jax.random.fold_in(jax.random.key(seed), part)
    key_x, key_t = jax.random.split(part_key)
    key_a, key_b = jax.random.split(jax.random.key(seed + 1))
    micro_in = jax.random.normal(key_x, (MICRO, TOKENS, D), jnp.float32)
    targets = jax.random.normal(key_t, (MICRO, TOKENS, D), jnp.float32)
    w_in = jax.random.normal(key_a, (STAGES, 2, D, FF), jnp.float32) * D ** -0.5
    w_out = jax.random.normal(key_b, (STAGES, 2, FF, D), jnp.float32) * (2.0 / (FF * STAGES)) ** 0.5
    return {'micro_in': micro_in.astype(jnp.bfloat16), 'targets': targets.astype(jnp.bfloat16), 'w_in': w_in.astype(jnp.bfloat16), 'w_out': w_out.astype(jnp.bfloat16)}


def gelu_pair(pre_f32):
    gelu_val, pull_fn = jax.vjp(jax.nn.gelu, pre_f32)
    return gelu_val, pull_fn(jnp.ones_like(pre_f32))[0]


def reference(micro_in, targets, w_in, w_out):
    layer_count = 2 * STAGES
    w_first = w_in.reshape(layer_count, D, FF)
    w_second = w_out.reshape(layer_count, FF, D)
    loss_scale = 1.0 / (MICRO * TOKENS * D)

    def layer_fwd(h_cur, weights):
        w_a, w_b = weights
        pre_act = jnp.dot(h_cur, w_a, preferred_element_type=jnp.float32).astype(jnp.bfloat16)
        act_val = jax.nn.gelu(pre_act.astype(jnp.float32)).astype(jnp.bfloat16)
        branch = jnp.dot(act_val, w_b, preferred_element_type=jnp.float32)
        return (h_cur.astype(jnp.float32) + branch).astype(jnp.bfloat16), (h_cur, pre_act)

    def layer_bwd(grad_h, layer_items):
        w_a, w_b, h_cur, pre_act = layer_items
        act_f32, gelu_slope = gelu_pair(pre_act.astype(jnp.float32))
        act_val = act_f32.astype(jnp.bfloat16)
        grad_act = jnp.dot(grad_h, w_b.T, preferred_element_type=jnp.float32)
        grad_pre = (gelu_slope * grad_act).astype(jnp.bfloat16)
        back_sum = jnp.dot(grad_pre, w_a.T, preferred_element_type=jnp.float32)
        grad_in = (grad_h.astype(jnp.float32) + back_sum).astype(jnp.bfloat16)
        grad_wa = jnp.dot(h_cur.T, grad_pre, preferred_element_type=jnp.float32)
        grad_wb = jnp.dot(act_val.T, grad_h, preferred_element_type=jnp.float32)
        return grad_in, (grad_wa, grad_wb)

    def one_micro(carry_state, micro_pair):
        acc_a, acc_b, loss_acc = carry_state
        x_now, tgt_now = micro_pair
        y_out, saved_acts = lax.scan(layer_fwd, x_now, (w_first, w_second))
        residual = y_out.astype(jnp.float32) - tgt_now.astype(jnp.float32)
        loss_acc = loss_acc + 0.5 * jnp.sum(residual * residual) * loss_scale
        grad_top = (residual * loss_scale).astype(jnp.bfloat16)
        grad_pair = lax.scan(layer_bwd, grad_top, (w_first, w_second, saved_acts[0], saved_acts[1]), reverse=True)[1]
        return (acc_a + grad_pair[0], acc_b + grad_pair[1], loss_acc), None

    init_state = (jnp.zeros((layer_count, D, FF), jnp.float32), jnp.zeros((layer_count, FF, D), jnp.float32), jnp.zeros((), jnp.float32))
    final_state = lax.scan(one_micro, init_state, (micro_in, targets))[0]
    acc_a, acc_b, loss_acc = final_state
    return acc_a.reshape(STAGES, 2, D, FF), acc_b.reshape(STAGES, 2, FF, D), loss_acc.reshape(1)
```

```python
import functools
import jax
import jax.numpy as jnp
from jax import lax
from jax.experimental import pallas as pl
from jax.experimental.pallas import tpu as pltpu
from jax.sharding import PartitionSpec as P

BF16 = jnp.bfloat16
F32 = jnp.float32
C0 = 0.7978845608028654
C1 = 0.044715 * C0
GROUP = 4
TILE = 256
RING = 20
SENDS = 4
SLOPE = 5
NEAR = 8


def gelu(x):
    return x * (0.5 + 0.5 * jnp.tanh(x * (C0 + C1 * (x * x))))


def gelu_pair(x):
    sq = x * x
    t = jnp.tanh(x * (C0 + C1 * sq))
    cdf = 0.5 + 0.5 * t
    slope = cdf + (x * (0.5 * C0 + 1.5 * C1 * sq)) * (1.0 - t * t)
    return x * cdf, slope


def tiles(width):
    return [slice(lo, lo + TILE) for lo in range(0, width, TILE)]


def kernel(stages, num_micro, ring, x_hbm, t_hbm, wa_hbm, wb_hbm, ga_out, gb_out, loss_out,
           wa, wb, wat, wbt, hh, uu, gg, ee, acc, act, et, hm, gm, gout, xt, lossv,
           f_recv, f_send, g_recv, g_send, w_sem, l_recv, l_send, o_sem):
    tokens, model = hh.shape[-2:]
    hidden = uu.shape[-1]
    me = lax.axis_index('stage')
    last = stages - 1
    is_last = me == last
    loss_scale = 1.0 / (num_micro * tokens * model)

    def weight_copies():
        return (pltpu.make_async_copy(wa_hbm, wa, w_sem.at[0]), pltpu.make_async_copy(wb_hbm, wb, w_sem.at[1]))

    for copy in weight_copies():
        copy.start()

    @pl.when(me == 0)
    def _():
        def load(j, c):
            pltpu.make_async_copy(x_hbm.at[j], hh.at[0, j], f_recv.at[j]).start()
            return c
        lax.fori_loop(0, num_micro, load, 0)

    @pl.when(is_last)
    def _():
        def load(j, c):
            pltpu.make_async_copy(t_hbm.at[j], gg.at[1, j], g_recv.at[j]).start()
            return c
        lax.fori_loop(0, num_micro, load, 0)
        lossv[...] = jnp.zeros_like(lossv)

    barrier = pltpu.get_barrier_semaphore()

    @pl.when(me > 0)
    def _():
        pl.semaphore_signal(barrier, inc=1, device_id={'stage': me - 1}, device_id_type=pl.DeviceIdType.MESH)

    @pl.when(me < last)
    def _():
        pl.semaphore_signal(barrier, inc=1, device_id={'stage': me + 1}, device_id_type=pl.DeviceIdType.MESH)

    pl.semaphore_wait(barrier, jnp.where((me == 0) | is_last, 1, 2))

    for copy in weight_copies():
        copy.wait()

    def send_fwd(j):
        return pltpu.make_async_remote_copy(
            src_ref=gg.at[0, j], dst_ref=hh.at[0, j], send_sem=f_send.at[j], recv_sem=f_recv.at[j],
            device_id={'stage': jnp.minimum(me + 1, last)}, device_id_type=pl.DeviceIdType.MESH)

    def send_bwd(i):
        slot = lax.rem(i, SENDS)
        return pltpu.make_async_remote_copy(
            src_ref=gout.at[slot], dst_ref=gg.at[1, i], send_sem=g_send.at[slot], recv_sem=g_recv.at[i],
            device_id={'stage': jnp.maximum(me - 1, 0)}, device_id_type=pl.DeviceIdType.MESH)

    def send_loss():
        return pltpu.make_async_remote_copy(
            src_ref=lossv, dst_ref=lossv, send_sem=l_send, recv_sem=l_recv,
            device_id={'stage': jnp.maximum(me - 1, 0)}, device_id_type=pl.DeviceIdType.MESH)

    def prepare():
        for l in range(2):
            for r in tiles(model):
                for c in tiles(hidden):
                    wat[l, c, r] = wa[l, r, c].T
                    wbt[l, r, c] = wb[l, c, r].T

        def clear(r, c):
            acc[r // (2 * model // 8), lax.rem(r // (model // 8), 2), pl.ds(lax.rem(r, model // 8) * 8, 8), :] = jnp.zeros((8, hidden), F32)
            return c
        lax.fori_loop(0, 4 * model // 8, clear, 0)

    def fwd_steps(j):
        def up(l, c):
            h = hh[0, j] if l == 0 else hm[...]
            pre = jnp.dot(h, wa[l, :, c], preferred_element_type=F32).astype(BF16)
            uu[l, j, :, c] = pre
            act[l, :, c] = gelu(pre.astype(F32)).astype(BF16)

        def down(l, c):
            h = hh[0, j, :, c] if l == 0 else hm[:, c]
            out = (h.astype(F32) + jnp.dot(act[l], wb[l, :, c], preferred_element_type=F32)).astype(BF16)
            if l == 0:
                hm[:, c] = out
                hh[1, j, :, c] = out
            else:
                gg[0, j, :, c] = out

        steps = []
        for l in range(2):
            steps.append([functools.partial(up, l, c) for c in tiles(hidden)])
            steps.append([functools.partial(down, l, c) for c in tiles(model)])
        return steps

    def bwd_steps(i):
        slot = lax.rem(i, ring)

        def up(l, c):
            g = gg[1, i] if l == 1 else gm[...]
            grad_act = jnp.dot(g, wbt[l, :, c], preferred_element_type=F32)
            val, slope = gelu_pair(uu[l, i, :, c].astype(F32))
            e = (slope * grad_act).astype(BF16)
            et[l, :, c] = e
            ee[l, slot, :, c] = e
            uu[l, i, :, c] = val.astype(BF16)

        def down(l, c):
            g = gg[1, i, :, c] if l == 1 else gm[:, c]
            out = (g.astype(F32) + jnp.dot(et[l], wat[l, :, c], preferred_element_type=F32)).astype(BF16)
            if l == 1:
                gm[:, c] = out
                gg[0, i, :, c] = out
            else:
                gout[lax.rem(i, SENDS), :, c] = out

        steps = []
        for l in (1, 0):
            steps.append([functools.partial(up, l, c) for c in tiles(hidden)])
            steps.append([functools.partial(down, l, c) for c in tiles(model)])
        return steps

    def wgt_steps(k):
        group = k // 4
        l = lax.rem(k // 2, 2)
        which = lax.rem(k, 2)
        return group, l, which

    def wgt(k, pick):
        group, l, _ = wgt_steps(k)
        first = group * GROUP
        rows = GROUP * tokens
        for r in tiles(rows):
            lo = first + r.start // tokens
            src = hh if pick == 0 else gg
            xt[:, r] = src[l, pl.ds(lo, TILE // tokens)].reshape(TILE, model).T
        out = []

        def piece(c):
            if pick == 0:
                y = ee[l, pl.ds(lax.rem(first, ring), GROUP), :, c]
            else:
                y = uu[l, pl.ds(first, GROUP), :, c]
            acc[pick, l, :, c] += jnp.dot(xt[...], y.reshape(rows, TILE), preferred_element_type=F32)

        return [functools.partial(piece, c) for c in tiles(hidden)]

    def run(*lists):
        for level in range(max(len(s) for s in lists)):
            parts = [s[level] for s in lists if level < len(s)]
            for at in range(max(len(p) for p in parts)):
                for p in parts:
                    if at < len(p):
                        p[at]()

    def wait_fwd(j):
        pltpu.make_async_copy(hh.at[0, j], hh.at[0, j], f_recv.at[j]).wait()

    def wait_bwd(i):
        @pl.when(is_last == False)
        def _():
            pltpu.make_async_copy(gg.at[1, i], gg.at[1, i], g_recv.at[i]).wait()
            send_fwd(i).wait_send()

        @pl.when((me > 0) & (i >= SENDS))
        def _():
            send_bwd(i - SENDS).wait_send()

    def ship_fwd(j):
        @pl.when(is_last == False)
        def _():
            send_fwd(j).start()

        @pl.when(is_last)
        def _():
            pltpu.make_async_copy(gg.at[1, j], gg.at[1, j], g_recv.at[j]).wait()
            res = gg[0, j].astype(F32) - gg[1, j].astype(F32)
            gg[1, j] = (res * loss_scale).astype(BF16)
            sq = jnp.sum((res * res).reshape(tokens // 8, 8, model), axis=0)
            part = sq[:, :128]
            for lo in range(128, model, 128):
                part = part + sq[:, lo:lo + 128]
            lossv[...] += part * (0.5 * loss_scale)

    def ship_bwd(i):
        @pl.when(me > 0)
        def _():
            send_bwd(i).start()

    warm = jnp.minimum(num_micro, 1 + SLOPE * (last - me))
    lag = jnp.where(me < NEAR, GROUP, ring - GROUP)
    prep_at = jnp.where(me == 0, num_micro, 0)

    def slot(t, carry):
        i = t - warm
        k = i - lag
        does_f = t < num_micro
        does_b = (i >= 0) & (i < num_micro)
        does_w = k >= 0
        which = lax.rem(k + 4, 2)

        @pl.when(t == prep_at)
        def _():
            prepare()

        @pl.when(i == num_micro - 1)
        def _():
            @pl.when(is_last == False)
            def _():
                pltpu.make_async_copy(lossv, lossv, l_recv).wait()

            @pl.when(me > 0)
            def _():
                send_loss().start()

        @pl.when(does_f)
        def _():
            wait_fwd(t)

        @pl.when(does_b)
        def _():
            wait_bwd(i)

        @pl.when(does_f & (i < 0))
        def _():
            run(fwd_steps(t))

        @pl.when(does_f & (i >= 0))
        def _():
            run(fwd_steps(t), bwd_steps(i))

        beside = does_b & (t >= num_micro)

        @pl.when(beside & (k < 0))
        def _():
            run(bwd_steps(i))

        for pick in range(2):
            @pl.when(beside & does_w & (which == pick))
            def _(pick=pick):
                pieces = wgt(k, pick)
                run(bwd_steps(i), [[p] for p in pieces])

        @pl.when(does_f)
        def _():
            ship_fwd(t)

        @pl.when(does_b)
        def _():
            ship_bwd(i)

        for pick in range(2):
            @pl.when(does_w & (beside == False) & (which == pick))
            def _(pick=pick):
                run([[p] for p in wgt(k, pick)])

        return carry

    lax.fori_loop(0, num_micro + warm + lag, slot, 0)

    outs = [pltpu.make_async_copy(acc.at[0], ga_out, o_sem.at[0]),
            pltpu.make_async_copy(acc.at[1], gb_out, o_sem.at[1]),
            pltpu.make_async_copy(lossv, loss_out, o_sem.at[2])]
    for copy in outs:
        copy.start()

    @pl.when(me > 0)
    def _():
        send_loss().wait_send()

        def drain(i, c):
            send_bwd(i).wait_send()
            return c
        lax.fori_loop(num_micro - SENDS, num_micro, drain, 0)

    for copy in outs:
        copy.wait()


def solution(mesh):
    stages = mesh.shape['stage']

    def per_device(micro_in, targets, w_in, w_out):
        num_micro, tokens, model = micro_in.shape
        hidden = w_in.shape[-1]
        ring = min(RING, num_micro)
        any_spec = pl.BlockSpec(memory_space=pl.ANY)
        dma = pltpu.SemaphoreType.DMA
        grad_a, grad_bt, loss = pl.pallas_call(
            functools.partial(kernel, stages, num_micro, ring),
            out_shape=(jax.ShapeDtypeStruct((2, model, hidden), F32), jax.ShapeDtypeStruct((2, model, hidden), F32), jax.ShapeDtypeStruct((8, 128), F32)),
            in_specs=[any_spec] * 4,
            out_specs=(any_spec,) * 3,
            scratch_shapes=[
                pltpu.VMEM((2, model, hidden), BF16),
                pltpu.VMEM((2, hidden, model), BF16),
                pltpu.VMEM((2, hidden, model), BF16),
                pltpu.VMEM((2, model, hidden), BF16),
                pltpu.VMEM((2, num_micro, tokens, model), BF16),
                pltpu.VMEM((2, num_micro, tokens, hidden), BF16),
                pltpu.VMEM((2, num_micro, tokens, model), BF16),
                pltpu.VMEM((2, ring, tokens, hidden), BF16),
                pltpu.VMEM((2, 2, model, hidden), F32),
                pltpu.VMEM((2, tokens, hidden), BF16),
                pltpu.VMEM((2, tokens, hidden), BF16),
                pltpu.VMEM((tokens, model), BF16),
                pltpu.VMEM((tokens, model), BF16),
                pltpu.VMEM((SENDS, tokens, model), BF16),
                pltpu.VMEM((model, GROUP * tokens), BF16),
                pltpu.VMEM((8, 128), F32),
                dma((num_micro,)), dma((num_micro,)), dma((num_micro,)), dma((SENDS,)),
                dma((2,)), dma(()), dma(()), dma((3,)),
            ],
            compiler_params=pltpu.CompilerParams(collective_id=0, has_side_effects=True, vmem_limit_bytes=67043328),
        )(micro_in, targets, w_in[0], w_out[0])
        return grad_a[None], jnp.swapaxes(grad_bt, 1, 2)[None], jnp.sum(loss).reshape(1)

    return jax.shard_map(per_device, mesh=mesh, in_specs=(P('data'), P('data'), P('stage'), P('stage')), out_specs=(P(('data', 'stage')), P(('data', 'stage')), P('data')), check_vma=False)
```

```python
import functools
import jax
import jax.numpy as jnp
from jax import lax
from jax.experimental import pallas as pl
from jax.experimental.pallas import tpu as pltpu
from jax.sharding import PartitionSpec as P

BF16 = jnp.bfloat16
F32 = jnp.float32
C0 = 0.7978845608028654
C1 = 0.044715 * C0
GROUP = 4
TILE = 256
RING = 24
SENDS = 4
SLOPE = 5
NEAR = 8
HALVES = 2
MIX = 0


def gelu(x):
    return x * (0.5 + 0.5 * jnp.tanh(x * (C0 + C1 * (x * x))))


def gelu_pair(x):
    sq = x * x
    t = jnp.tanh(x * (C0 + C1 * sq))
    cdf = 0.5 + 0.5 * t
    slope = cdf + (x * (0.5 * C0 + 1.5 * C1 * sq)) * (1.0 - t * t)
    return x * cdf, slope


def tiles(width):
    return [slice(lo, lo + TILE) for lo in range(0, width, TILE)]


def kernel(stages, num_micro, ring, x_hbm, t_hbm, wa_hbm, wb_hbm, ga_out, gb_out, loss_out,
           wa, wb, wat, wbt, hh, uu, gg, ee, acc, act, et, hm, gm, gout, xt, lossv,
           f_recv, f_send, g_recv, g_send, w_sem, l_recv, l_send, o_sem):
    tokens, model = hh.shape[-2:]
    hidden = uu.shape[-1]
    me = lax.axis_index('stage')
    last = stages - 1
    is_last = me == last
    loss_scale = 1.0 / (num_micro * tokens * model)

    half = tokens // HALVES

    def part(m):
        return m // HALVES, pl.ds(pl.multiple_of(lax.rem(m, HALVES) * half, half), half)

    def weight_copies():
        return (pltpu.make_async_copy(wa_hbm, wa, w_sem.at[0]), pltpu.make_async_copy(wb_hbm, wb, w_sem.at[1]))

    for copy in weight_copies():
        copy.start()

    @pl.when(me == 0)
    def _():
        def load(m, c):
            j, rows = part(m)
            pltpu.make_async_copy(x_hbm.at[j, rows], hh.at[0, j, rows], f_recv.at[m]).start()
            return c
        lax.fori_loop(0, num_micro * HALVES, load, 0)

    @pl.when(is_last)
    def _():
        def load(m, c):
            j, rows = part(m)
            pltpu.make_async_copy(t_hbm.at[j, rows], gg.at[1, j, rows], g_recv.at[m]).start()
            return c
        lax.fori_loop(0, num_micro * HALVES, load, 0)
        lossv[...] = jnp.zeros_like(lossv)

    barrier = pltpu.get_barrier_semaphore()

    @pl.when(me > 0)
    def _():
        pl.semaphore_signal(barrier, inc=1, device_id={'stage': me - 1}, device_id_type=pl.DeviceIdType.MESH)

    @pl.when(me < last)
    def _():
        pl.semaphore_signal(barrier, inc=1, device_id={'stage': me + 1}, device_id_type=pl.DeviceIdType.MESH)

    pl.semaphore_wait(barrier, jnp.where((me == 0) | is_last, 1, 2))

    for copy in weight_copies():
        copy.wait()

    def send_fwd(m):
        j, rows = part(m)
        return pltpu.make_async_remote_copy(
            src_ref=gg.at[0, j, rows], dst_ref=hh.at[0, j, rows], send_sem=f_send.at[m], recv_sem=f_recv.at[m],
            device_id={'stage': jnp.minimum(me + 1, last)}, device_id_type=pl.DeviceIdType.MESH)

    def send_bwd(m):
        i, rows = part(m)
        return pltpu.make_async_remote_copy(
            src_ref=gout.at[lax.rem(i, SENDS), rows], dst_ref=gg.at[1, i, rows],
            send_sem=g_send.at[lax.rem(m, SENDS * HALVES)], recv_sem=g_recv.at[m],
            device_id={'stage': jnp.maximum(me - 1, 0)}, device_id_type=pl.DeviceIdType.MESH)

    def send_loss():
        return pltpu.make_async_remote_copy(
            src_ref=lossv, dst_ref=lossv, send_sem=l_send, recv_sem=l_recv,
            device_id={'stage': jnp.maximum(me - 1, 0)}, device_id_type=pl.DeviceIdType.MESH)

    def prepare():
        for l in range(2):
            for r in tiles(model):
                for c in tiles(hidden):
                    wat[l, c, r] = wa[l, r, c].T
                    wbt[l, r, c] = wb[l, c, r].T

        def clear(r, c):
            acc[r // (2 * model // 8), lax.rem(r // (model // 8), 2), pl.ds(lax.rem(r, model // 8) * 8, 8), :] = jnp.zeros((8, hidden), F32)
            return c
        lax.fori_loop(0, 4 * model // 8, clear, 0)

    def fwd_steps(j, rows, n):
        def up(l, c):
            h = hh[0, j, rows] if l == 0 else hm[:n]
            pre = jnp.dot(h, wa[l, :, c], preferred_element_type=F32).astype(BF16)
            uu[l, j, rows, c] = pre
            act[l, :n, c] = gelu(pre.astype(F32)).astype(BF16)

        def down(l, c):
            h = hh[0, j, rows, c] if l == 0 else hm[:n, c]
            out = (h.astype(F32) + jnp.dot(act[l, :n], wb[l, :, c], preferred_element_type=F32)).astype(BF16)
            if l == 0:
                hm[:n, c] = out
                hh[1, j, rows, c] = out
            else:
                gg[0, j, rows, c] = out

        steps = []
        for l in range(2):
            steps.append([functools.partial(up, l, c) for c in tiles(hidden)])
            steps.append([functools.partial(down, l, c) for c in tiles(model)])
        return steps

    def bwd_steps(i, rows, n):
        slot = lax.rem(i, ring)

        def up(l, c):
            g = gg[1, i, rows] if l == 1 else gm[:n]
            grad_act = jnp.dot(g, wbt[l, :, c], preferred_element_type=F32)
            val, slope = gelu_pair(uu[l, i, rows, c].astype(F32))
            e = (slope * grad_act).astype(BF16)
            et[l, :n, c] = e
            ee[l, slot, rows, c] = e
            uu[l, i, rows, c] = val.astype(BF16)

        def down(l, c):
            g = gg[1, i, rows, c] if l == 1 else gm[:n, c]
            out = (g.astype(F32) + jnp.dot(et[l, :n], wat[l, :, c], preferred_element_type=F32)).astype(BF16)
            if l == 1:
                gm[:n, c] = out
                gg[0, i, rows, c] = out
            else:
                gout[lax.rem(i, SENDS), rows, c] = out

        steps = []
        for l in (1, 0):
            steps.append([functools.partial(up, l, c) for c in tiles(hidden)])
            steps.append([functools.partial(down, l, c) for c in tiles(model)])
        return steps

    def wgt(k, pick):
        l = lax.rem(k // 2, 2)
        first = (k // 4) * GROUP
        rows = GROUP * tokens
        for r in tiles(rows):
            lo = first + r.start // tokens
            src = hh if pick == 0 else gg
            xt[:, r] = src[l, pl.ds(lo, TILE // tokens)].reshape(TILE, model).T
        out = []

        def piece(c):
            if pick == 0:
                y = ee[l, pl.ds(lax.rem(first, ring), GROUP), :, c]
            else:
                y = uu[l, pl.ds(first, GROUP), :, c]
            acc[pick, l, :, c] += jnp.dot(xt[...], y.reshape(rows, TILE), preferred_element_type=F32)

        return [functools.partial(piece, c) for c in tiles(hidden)]

    def run(*lists):
        if MIX == 0:
            lists = [sum(lists, [])]
        for level in range(max(len(s) for s in lists)):
            parts = [s[level] for s in lists if level < len(s)]
            if MIX < 2:
                parts = [sum(parts, [])]
            for at in range(max(len(p) for p in parts)):
                for p in parts:
                    if at < len(p):
                        p[at]()

    def wait_fwd(m):
        j, rows = part(m)
        pltpu.make_async_copy(hh.at[0, j, rows], hh.at[0, j, rows], f_recv.at[m]).wait()

    def wait_bwd(m):
        i, rows = part(m)

        @pl.when(is_last == False)
        def _():
            pltpu.make_async_copy(gg.at[1, i, rows], gg.at[1, i, rows], g_recv.at[m]).wait()
            send_fwd(m).wait_send()

        @pl.when((me > 0) & (m >= SENDS * HALVES))
        def _():
            send_bwd(m - SENDS * HALVES).wait_send()

    def ship_fwd(m):
        j, rows = part(m)

        @pl.when(is_last == False)
        def _():
            send_fwd(m).start()

        @pl.when(is_last)
        def _():
            pltpu.make_async_copy(gg.at[1, j, rows], gg.at[1, j, rows], g_recv.at[m]).wait()
            res = gg[0, j, rows].astype(F32) - gg[1, j, rows].astype(F32)
            gg[1, j, rows] = (res * loss_scale).astype(BF16)
            sq = jnp.sum((res * res).reshape(half // 8, 8, model), axis=0)
            total = sq[:, :128]
            for lo in range(128, model, 128):
                total = total + sq[:, lo:lo + 128]
            lossv[...] += total * (0.5 * loss_scale)

    def ship_bwd(m):
        @pl.when(me > 0)
        def _():
            send_bwd(m).start()

    def each(j, body):
        def step(b, c):
            body(j * HALVES + b)
            return c
        lax.fori_loop(0, HALVES, step, 0)

    warm = jnp.minimum(num_micro, 1 + SLOPE * (last - me))
    lag = jnp.where(me < NEAR, GROUP, ring - GROUP)
    prep_at = jnp.where(me == 0, num_micro, 0)

    def slot(t, carry):
        i = t - warm
        k = i - lag
        does_f = t < num_micro
        does_b = (i >= 0) & (i < num_micro)
        does_w = k >= 0
        which = lax.rem(k + 4, 2)

        @pl.when(t == prep_at)
        def _():
            prepare()

        @pl.when(i == num_micro - 1)
        def _():
            @pl.when(is_last == False)
            def _():
                pltpu.make_async_copy(lossv, lossv, l_recv).wait()

            @pl.when(me > 0)
            def _():
                send_loss().start()

        @pl.when(does_f & (i < 0))
        def _():
            def step(m):
                wait_fwd(m)
                run(fwd_steps(*part(m), half))
                ship_fwd(m)
            each(t, step)

        @pl.when(does_f & (i >= 0))
        def _():
            rows = slice(None)
            each(t, wait_fwd)
            each(i, wait_bwd)
            run(fwd_steps(t, rows, tokens), bwd_steps(i, rows, tokens))
            each(i, ship_bwd)
            each(t, ship_fwd)

        @pl.when(does_b & (t >= num_micro))
        def _():
            def step(m):
                wait_bwd(m)
                run(bwd_steps(*part(m), half))
                ship_bwd(m)
            each(i, step)

        for pick in range(2):
            @pl.when(does_w & (which == pick))
            def _(pick=pick):
                for piece in wgt(k, pick):
                    piece()

        return carry

    lax.fori_loop(0, num_micro + warm + lag, slot, 0)

    outs = [pltpu.make_async_copy(acc.at[0], ga_out, o_sem.at[0]),
            pltpu.make_async_copy(acc.at[1], gb_out, o_sem.at[1]),
            pltpu.make_async_copy(lossv, loss_out, o_sem.at[2])]
    for copy in outs:
        copy.start()

    @pl.when(me > 0)
    def _():
        send_loss().wait_send()

        def drain(m, c):
            send_bwd(m).wait_send()
            return c
        lax.fori_loop((num_micro - SENDS) * HALVES, num_micro * HALVES, drain, 0)

    for copy in outs:
        copy.wait()


def solution(mesh):
    stages = mesh.shape['stage']

    def per_device(micro_in, targets, w_in, w_out):
        num_micro, tokens, model = micro_in.shape
        hidden = w_in.shape[-1]
        ring = min(RING, num_micro)
        any_spec = pl.BlockSpec(memory_space=pl.ANY)
        dma = pltpu.SemaphoreType.DMA
        grad_a, grad_bt, loss = pl.pallas_call(
            functools.partial(kernel, stages, num_micro, ring),
            out_shape=(jax.ShapeDtypeStruct((2, model, hidden), F32), jax.ShapeDtypeStruct((2, model, hidden), F32), jax.ShapeDtypeStruct((8, 128), F32)),
            in_specs=[any_spec] * 4,
            out_specs=(any_spec,) * 3,
            scratch_shapes=[
                pltpu.VMEM((2, model, hidden), BF16),
                pltpu.VMEM((2, hidden, model), BF16),
                pltpu.VMEM((2, hidden, model), BF16),
                pltpu.VMEM((2, model, hidden), BF16),
                pltpu.VMEM((2, num_micro, tokens, model), BF16),
                pltpu.VMEM((2, num_micro, tokens, hidden), BF16),
                pltpu.VMEM((2, num_micro, tokens, model), BF16),
                pltpu.VMEM((2, ring, tokens, hidden), BF16),
                pltpu.VMEM((2, 2, model, hidden), F32),
                pltpu.VMEM((2, tokens, hidden), BF16),
                pltpu.VMEM((2, tokens, hidden), BF16),
                pltpu.VMEM((tokens, model), BF16),
                pltpu.VMEM((tokens, model), BF16),
                pltpu.VMEM((SENDS, tokens, model), BF16),
                pltpu.VMEM((model, GROUP * tokens), BF16),
                pltpu.VMEM((8, 128), F32),
                dma((num_micro * HALVES,)), dma((num_micro * HALVES,)), dma((num_micro * HALVES,)), dma((SENDS * HALVES,)),
                dma((2,)), dma(()), dma(()), dma((3,)),
            ],
            compiler_params=pltpu.CompilerParams(collective_id=0, has_side_effects=True, vmem_limit_bytes=67043328),
        )(micro_in, targets, w_in[0], w_out[0])
        return grad_a[None], jnp.swapaxes(grad_bt, 1, 2)[None], jnp.sum(loss).reshape(1)

    return jax.shard_map(per_device, mesh=mesh, in_specs=(P('data'), P('data'), P('stage'), P('stage')), out_specs=(P(('data', 'stage')), P(('data', 'stage')), P('data')), check_vma=False)
```

```python
import functools
import jax
import jax.numpy as jnp
from jax import lax
from jax.experimental import pallas as pl
from jax.experimental.pallas import tpu as pltpu
from jax.sharding import PartitionSpec as P

BF16 = jnp.bfloat16
F32 = jnp.float32
C0 = 0.7978845608028654
C1 = 0.044715 * C0
GROUP = 4
TILE = 256
RING = 8
SENDS = 4
PAIR_SLACK = 3
CHIP_SLACK = 7
NEAR = 8
HALVES = 2


def gelu(x):
    return x * (0.5 + 0.5 * jnp.tanh(x * (C0 + C1 * (x * x))))


def gelu_pair(x):
    sq = x * x
    t = jnp.tanh(x * (C0 + C1 * sq))
    cdf = 0.5 + 0.5 * t
    slope = cdf + (x * (0.5 * C0 + 1.5 * C1 * sq)) * (1.0 - t * t)
    return x * cdf, slope


def tiles(width):
    return [slice(lo, lo + TILE) for lo in range(0, width, TILE)]


def kernel(stages, num_micro, ring, x_hbm, t_hbm, wa_hbm, wb_hbm, ga_out, gb_out, loss_out, e_hbm,
           wa, wb, wat, wbt, hh, uu, gg, ee, es, acc, act, et, hm, gm, gout, xt, lossv,
           f_recv, f_send, g_recv, g_send, w_sem, l_recv, l_send, o_sem, e_out, e_in):
    tokens, model = hh.shape[-2:]
    hidden = uu.shape[-1]
    me = lax.axis_index('stage')
    last = stages - 1
    is_last = me == last
    loss_scale = 1.0 / (num_micro * tokens * model)

    half = tokens // HALVES

    def part(m):
        return m // HALVES, pl.ds(pl.multiple_of(lax.rem(m, HALVES) * half, half), half)

    def weight_copies():
        return (pltpu.make_async_copy(wa_hbm, wa, w_sem.at[0]), pltpu.make_async_copy(wb_hbm, wb, w_sem.at[1]))

    for copy in weight_copies():
        copy.start()

    @pl.when(me == 0)
    def _():
        def load(m, c):
            j, rows = part(m)
            pltpu.make_async_copy(x_hbm.at[j, rows], hh.at[0, j, rows], f_recv.at[m]).start()
            return c
        lax.fori_loop(0, num_micro * HALVES, load, 0)

    @pl.when(is_last)
    def _():
        def load(m, c):
            j, rows = part(m)
            pltpu.make_async_copy(t_hbm.at[j, rows], gg.at[1, j, rows], g_recv.at[m]).start()
            return c
        lax.fori_loop(0, num_micro * HALVES, load, 0)
        lossv[...] = jnp.zeros_like(lossv)

    barrier = pltpu.get_barrier_semaphore()

    @pl.when(me > 0)
    def _():
        pl.semaphore_signal(barrier, inc=1, device_id={'stage': me - 1}, device_id_type=pl.DeviceIdType.MESH)

    @pl.when(me < last)
    def _():
        pl.semaphore_signal(barrier, inc=1, device_id={'stage': me + 1}, device_id_type=pl.DeviceIdType.MESH)

    pl.semaphore_wait(barrier, jnp.where((me == 0) | is_last, 1, 2))

    for copy in weight_copies():
        copy.wait()

    def send_fwd(m):
        j, rows = part(m)
        return pltpu.make_async_remote_copy(
            src_ref=gg.at[0, j, rows], dst_ref=hh.at[0, j, rows], send_sem=f_send.at[m], recv_sem=f_recv.at[m],
            device_id={'stage': jnp.minimum(me + 1, last)}, device_id_type=pl.DeviceIdType.MESH)

    def send_bwd(m):
        i, rows = part(m)
        return pltpu.make_async_remote_copy(
            src_ref=gout.at[lax.rem(i, SENDS), rows], dst_ref=gg.at[1, i, rows],
            send_sem=g_send.at[lax.rem(m, SENDS * HALVES)], recv_sem=g_recv.at[m],
            device_id={'stage': jnp.maximum(me - 1, 0)}, device_id_type=pl.DeviceIdType.MESH)

    def send_loss():
        return pltpu.make_async_remote_copy(
            src_ref=lossv, dst_ref=lossv, send_sem=l_send, recv_sem=l_recv,
            device_id={'stage': jnp.maximum(me - 1, 0)}, device_id_type=pl.DeviceIdType.MESH)

    def prepare():
        for l in range(2):
            for r in tiles(model):
                for c in tiles(hidden):
                    wat[l, c, r] = wa[l, r, c].T
                    wbt[l, r, c] = wb[l, c, r].T

        def clear(r, c):
            acc[r // (2 * model // 8), lax.rem(r // (model // 8), 2), pl.ds(lax.rem(r, model // 8) * 8, 8), :] = jnp.zeros((8, hidden), F32)
            return c
        lax.fori_loop(0, 4 * model // 8, clear, 0)

    def fwd_steps(j, rows, n):
        def up(l, c):
            h = hh[0, j, rows] if l == 0 else hm[:n]
            pre = jnp.dot(h, wa[l, :, c], preferred_element_type=F32).astype(BF16)
            uu[l, j, rows, c] = pre
            act[l, :n, c] = gelu(pre.astype(F32)).astype(BF16)

        def down(l, c):
            h = hh[0, j, rows, c] if l == 0 else hm[:n, c]
            out = (h.astype(F32) + jnp.dot(act[l, :n], wb[l, :, c], preferred_element_type=F32)).astype(BF16)
            if l == 0:
                hm[:n, c] = out
                hh[1, j, rows, c] = out
            else:
                gg[0, j, rows, c] = out

        steps = []
        for l in range(2):
            steps.append([functools.partial(up, l, c) for c in tiles(hidden)])
            steps.append([functools.partial(down, l, c) for c in tiles(model)])
        return steps

    def bwd_steps(i, rows, n):
        slot = lax.rem(i, ring)

        def up(l, c):
            g = gg[1, i, rows] if l == 1 else gm[:n]
            grad_act = jnp.dot(g, wbt[l, :, c], preferred_element_type=F32)
            val, slope = gelu_pair(uu[l, i, rows, c].astype(F32))
            e = (slope * grad_act).astype(BF16)
            et[l, :n, c] = e
            ee[l, slot, rows, c] = e
            uu[l, i, rows, c] = val.astype(BF16)

        def down(l, c):
            g = gg[1, i, rows, c] if l == 1 else gm[:n, c]
            out = (g.astype(F32) + jnp.dot(et[l, :n], wat[l, :, c], preferred_element_type=F32)).astype(BF16)
            if l == 1:
                gm[:n, c] = out
                gg[0, i, rows, c] = out
            else:
                gout[lax.rem(i, SENDS), rows, c] = out

        steps = []
        for l in (1, 0):
            steps.append([functools.partial(up, l, c) for c in tiles(hidden)])
            steps.append([functools.partial(down, l, c) for c in tiles(model)])
        return steps

    def store_e(i):
        slot = lax.rem(i, ring)
        return pltpu.make_async_copy(ee.at[:, slot], e_hbm.at[:, i], e_out.at[slot])

    def load_e(k):
        l, first, buf = lax.rem(k // 2, 2), (k // 4) * GROUP, lax.rem(k // 2, 2)
        return pltpu.make_async_copy(e_hbm.at[l, pl.ds(first, GROUP)], es.at[buf], e_in.at[buf])

    def result(k, pick):
        l = lax.rem(k // 2, 2)
        return pltpu.make_async_copy(acc.at[pick, l], (ga_out, gb_out)[pick].at[l], o_sem.at[pick, l])

    def wgt(k, pick, direct):
        l = lax.rem(k // 2, 2)
        first = (k // 4) * GROUP
        rows = GROUP * tokens
        for r in tiles(rows):
            lo = first + r.start // tokens
            src = hh if pick == 0 else gg
            xt[:, r] = src[l, pl.ds(lo, TILE // tokens)].reshape(TILE, model).T

        def piece(c):
            if pick == 0 and direct:
                y = ee[l, pl.ds(lax.rem(first, ring), GROUP), :, c]
            elif pick == 0:
                y = es[lax.rem(k // 2, 2), :, :, c]
            else:
                y = uu[l, pl.ds(first, GROUP), :, c]
            acc[pick, l, :, c] += jnp.dot(xt[...], y.reshape(rows, TILE), preferred_element_type=F32)

        for c in tiles(hidden):
            piece(c)

    def run(*lists):
        for steps in lists:
            for pieces in steps:
                for piece in pieces:
                    piece()

    def wait_fwd(m):
        j, rows = part(m)
        pltpu.make_async_copy(hh.at[0, j, rows], hh.at[0, j, rows], f_recv.at[m]).wait()

    def wait_bwd(m):
        i, rows = part(m)

        @pl.when(is_last == False)
        def _():
            pltpu.make_async_copy(gg.at[1, i, rows], gg.at[1, i, rows], g_recv.at[m]).wait()
            send_fwd(m).wait_send()

        @pl.when((me > 0) & (m >= SENDS * HALVES))
        def _():
            send_bwd(m - SENDS * HALVES).wait_send()

    def ship_fwd(m):
        j, rows = part(m)

        @pl.when(is_last == False)
        def _():
            send_fwd(m).start()

        @pl.when(is_last)
        def _():
            pltpu.make_async_copy(gg.at[1, j, rows], gg.at[1, j, rows], g_recv.at[m]).wait()
            res = gg[0, j, rows].astype(F32) - gg[1, j, rows].astype(F32)
            gg[1, j, rows] = (res * loss_scale).astype(BF16)
            sq = jnp.sum((res * res).reshape(half // 8, 8, model), axis=0)
            total = sq[:, :128]
            for lo in range(128, model, 128):
                total = total + sq[:, lo:lo + 128]
            lossv[...] += total * (0.5 * loss_scale)

    def ship_bwd(m):
        @pl.when(me > 0)
        def _():
            send_bwd(m).start()

    def each(j, body):
        def step(b, c):
            body(j * HALVES + b)
            return c
        lax.fori_loop(0, HALVES, step, 0)

    warm = jnp.minimum(num_micro, 1 + PAIR_SLACK * ((last - me + 1) // 2) + CHIP_SLACK * ((last - me) // 2))
    near = me < NEAR
    lag = jnp.where(near, GROUP, num_micro)
    prep_at = jnp.where(me == 0, num_micro, 0)

    def slot(t, carry):
        i = t - warm
        k = i - lag
        does_f = t < num_micro
        does_b = (i >= 0) & (i < num_micro)
        does_w = k >= 0
        which = lax.rem(k + 2 * num_micro, 2)

        @pl.when(t == prep_at)
        def _():
            prepare()

        @pl.when(i == num_micro - 1)
        def _():
            @pl.when(is_last == False)
            def _():
                pltpu.make_async_copy(lossv, lossv, l_recv).wait()

            @pl.when(me > 0)
            def _():
                send_loss().start()

        @pl.when(does_f & (i < 0))
        def _():
            def step(m):
                wait_fwd(m)
                run(fwd_steps(*part(m), half))
                ship_fwd(m)
            each(t, step)

        @pl.when(does_f & (i >= 0))
        def _():
            rows = slice(None)
            each(t, wait_fwd)
            each(i, wait_bwd)
            run(fwd_steps(t, rows, tokens), bwd_steps(i, rows, tokens))
            each(i, ship_bwd)
            each(t, ship_fwd)

        @pl.when(does_b & (t >= num_micro))
        def _():
            def step(m):
                wait_bwd(m)
                run(bwd_steps(*part(m), half))
                ship_bwd(m)
            each(i, step)

        @pl.when(does_b & (near == False))
        def _():
            store_e(i).start()

            @pl.when(i > 0)
            def _():
                store_e(i - 1).wait()

        @pl.when((i == num_micro) & (near == False))
        def _():
            store_e(num_micro - 1).wait()
            load_e(0).start()

        @pl.when(does_w & (which == 0) & near)
        def _():
            wgt(k, 0, True)

        @pl.when(does_w & (which == 0) & (near == False))
        def _():
            @pl.when(k + 2 < num_micro)
            def _():
                load_e(k + 2).start()
            load_e(k).wait()
            wgt(k, 0, False)

        @pl.when(does_w & (which == 1))
        def _():
            wgt(k, 1, True)

        for pick in range(2):
            @pl.when((k >= num_micro - 4) & (which == pick))
            def _(pick=pick):
                result(k, pick).start()

        return carry

    lax.fori_loop(0, num_micro + warm + lag, slot, 0)

    loss_copy = pltpu.make_async_copy(lossv, loss_out, e_in.at[0])
    loss_copy.start()

    @pl.when(me > 0)
    def _():
        send_loss().wait_send()

        def drain(m, c):
            send_bwd(m).wait_send()
            return c
        lax.fori_loop((num_micro - SENDS) * HALVES, num_micro * HALVES, drain, 0)

    loss_copy.wait()
    for k in range(4):
        result(k, k % 2).wait()


def solution(mesh):
    stages = mesh.shape['stage']

    def per_device(micro_in, targets, w_in, w_out):
        num_micro, tokens, model = micro_in.shape
        hidden = w_in.shape[-1]
        ring = min(RING, num_micro)
        any_spec = pl.BlockSpec(memory_space=pl.ANY)
        dma = pltpu.SemaphoreType.DMA
        grad_a, grad_bt, loss, _ = pl.pallas_call(
            functools.partial(kernel, stages, num_micro, ring),
            out_shape=(jax.ShapeDtypeStruct((2, model, hidden), F32), jax.ShapeDtypeStruct((2, model, hidden), F32), jax.ShapeDtypeStruct((8, 128), F32), jax.ShapeDtypeStruct((2, num_micro, tokens, hidden), BF16)),
            in_specs=[any_spec] * 4,
            out_specs=(any_spec,) * 4,
            scratch_shapes=[
                pltpu.VMEM((2, model, hidden), BF16),
                pltpu.VMEM((2, hidden, model), BF16),
                pltpu.VMEM((2, hidden, model), BF16),
                pltpu.VMEM((2, model, hidden), BF16),
                pltpu.VMEM((2, num_micro, tokens, model), BF16),
                pltpu.VMEM((2, num_micro, tokens, hidden), BF16),
                pltpu.VMEM((2, num_micro, tokens, model), BF16),
                pltpu.VMEM((2, ring, tokens, hidden), BF16),
                pltpu.VMEM((2, GROUP, tokens, hidden), BF16),
                pltpu.VMEM((2, 2, model, hidden), F32),
                pltpu.VMEM((2, tokens, hidden), BF16),
                pltpu.VMEM((2, tokens, hidden), BF16),
                pltpu.VMEM((tokens, model), BF16),
                pltpu.VMEM((tokens, model), BF16),
                pltpu.VMEM((SENDS, tokens, model), BF16),
                pltpu.VMEM((model, GROUP * tokens), BF16),
                pltpu.VMEM((8, 128), F32),
                dma((num_micro * HALVES,)), dma((num_micro * HALVES,)), dma((num_micro * HALVES,)), dma((SENDS * HALVES,)),
                dma((2,)), dma(()), dma(()), dma((2, 2)), dma((ring,)), dma((2,)),
            ],
            compiler_params=pltpu.CompilerParams(collective_id=0, has_side_effects=True, vmem_limit_bytes=67043328),
        )(micro_in, targets, w_in[0], w_out[0])
        return grad_a[None], jnp.swapaxes(grad_bt, 1, 2)[None], jnp.sum(loss).reshape(1)

    return jax.shard_map(per_device, mesh=mesh, in_specs=(P('data'), P('data'), P('stage'), P('stage')), out_specs=(P(('data', 'stage')), P(('data', 'stage')), P('data')), check_vma=False)
```

```python
import functools
import jax
import jax.numpy as jnp
from jax import lax
from jax.experimental import pallas as pl
from jax.experimental.pallas import tpu as pltpu
from jax.sharding import PartitionSpec as P

BF16 = jnp.bfloat16
F32 = jnp.float32
C0 = 0.7978845608028654
C1 = 0.044715 * C0
GROUP = 4
TILE = 256
RING = 8
SENDS = 4
PAIR_SLACK = 3
CHIP_SLACK = 5
NEAR = 8
HALVES = 2


def gelu(x):
    return x * (0.5 + 0.5 * jnp.tanh(x * (C0 + C1 * (x * x))))


def gelu_pair(x):
    sq = x * x
    t = jnp.tanh(x * (C0 + C1 * sq))
    cdf = 0.5 + 0.5 * t
    slope = cdf + (x * (0.5 * C0 + 1.5 * C1 * sq)) * (1.0 - t * t)
    return x * cdf, slope


def tiles(width):
    return [slice(lo, lo + TILE) for lo in range(0, width, TILE)]


def kernel(stages, num_micro, ring, x_hbm, t_hbm, wa_hbm, wb_hbm, ga_out, gb_out, loss_out, e_hbm,
           wa, wb, wat, wbt, hh, uu, gg, ee, es, acc, act, et, hm, gm, gout, xt, lossv,
           f_recv, f_send, g_recv, g_send, w_sem, l_recv, l_send, o_sem, e_out, e_in):
    tokens, model = hh.shape[-2:]
    hidden = uu.shape[-1]
    me = lax.axis_index('stage')
    last = stages - 1
    is_last = me == last
    loss_scale = 1.0 / (num_micro * tokens * model)

    half = tokens // HALVES

    def part(m):
        return m // HALVES, pl.ds(pl.multiple_of(lax.rem(m, HALVES) * half, half), half)

    def weight_copies():
        return (pltpu.make_async_copy(wa_hbm, wa, w_sem.at[0]), pltpu.make_async_copy(wb_hbm, wb, w_sem.at[1]))

    for copy in weight_copies():
        copy.start()

    @pl.when(me == 0)
    def _():
        def load(m, c):
            j, rows = part(m)
            pltpu.make_async_copy(x_hbm.at[j, rows], hh.at[0, j, rows], f_recv.at[m]).start()
            return c
        lax.fori_loop(0, num_micro * HALVES, load, 0)

    @pl.when(is_last)
    def _():
        def load(m, c):
            j, rows = part(m)
            pltpu.make_async_copy(t_hbm.at[j, rows], gg.at[1, j, rows], g_recv.at[m]).start()
            return c
        lax.fori_loop(0, num_micro * HALVES, load, 0)
        lossv[...] = jnp.zeros_like(lossv)

    barrier = pltpu.get_barrier_semaphore()

    @pl.when(me > 0)
    def _():
        pl.semaphore_signal(barrier, inc=1, device_id={'stage': me - 1}, device_id_type=pl.DeviceIdType.MESH)

    @pl.when(me < last)
    def _():
        pl.semaphore_signal(barrier, inc=1, device_id={'stage': me + 1}, device_id_type=pl.DeviceIdType.MESH)

    pl.semaphore_wait(barrier, jnp.where((me == 0) | is_last, 1, 2))

    for copy in weight_copies():
        copy.wait()

    def send_fwd(m):
        j, rows = part(m)
        return pltpu.make_async_remote_copy(
            src_ref=gg.at[0, j, rows], dst_ref=hh.at[0, j, rows], send_sem=f_send.at[m], recv_sem=f_recv.at[m],
            device_id={'stage': jnp.minimum(me + 1, last)}, device_id_type=pl.DeviceIdType.MESH)

    def send_bwd(m):
        i, rows = part(m)
        return pltpu.make_async_remote_copy(
            src_ref=gout.at[lax.rem(i, SENDS), rows], dst_ref=gg.at[1, i, rows],
            send_sem=g_send.at[lax.rem(m, SENDS * HALVES)], recv_sem=g_recv.at[m],
            device_id={'stage': jnp.maximum(me - 1, 0)}, device_id_type=pl.DeviceIdType.MESH)

    def send_loss():
        return pltpu.make_async_remote_copy(
            src_ref=lossv, dst_ref=lossv, send_sem=l_send, recv_sem=l_recv,
            device_id={'stage': jnp.maximum(me - 1, 0)}, device_id_type=pl.DeviceIdType.MESH)

    def prepare():
        for l in range(2):
            for r in tiles(model):
                for c in tiles(hidden):
                    wat[l, c, r] = wa[l, r, c].T
                    wbt[l, r, c] = wb[l, c, r].T

        def clear(r, c):
            acc[r // (2 * model // 8), lax.rem(r // (model // 8), 2), pl.ds(lax.rem(r, model // 8) * 8, 8), :] = jnp.zeros((8, hidden), F32)
            return c
        lax.fori_loop(0, 4 * model // 8, clear, 0)

    def fwd_steps(j, rows, n):
        def up(l, c):
            h = hh[0, j, rows] if l == 0 else hm[:n]
            pre = jnp.dot(h, wa[l, :, c], preferred_element_type=F32).astype(BF16)
            uu[l, j, rows, c] = pre
            act[l, :n, c] = gelu(pre.astype(F32)).astype(BF16)

        def down(l, c):
            h = hh[0, j, rows, c] if l == 0 else hm[:n, c]
            out = (h.astype(F32) + jnp.dot(act[l, :n], wb[l, :, c], preferred_element_type=F32)).astype(BF16)
            if l == 0:
                hm[:n, c] = out
                hh[1, j, rows, c] = out
            else:
                gg[0, j, rows, c] = out

        steps = []
        for l in range(2):
            steps.append([functools.partial(up, l, c) for c in tiles(hidden)])
            steps.append([functools.partial(down, l, c) for c in tiles(model)])
        return steps

    def bwd_steps(i, rows, n):
        slot = lax.rem(i, ring)

        def up(l, c):
            g = gg[1, i, rows] if l == 1 else gm[:n]
            grad_act = jnp.dot(g, wbt[l, :, c], preferred_element_type=F32)
            val, slope = gelu_pair(uu[l, i, rows, c].astype(F32))
            e = (slope * grad_act).astype(BF16)
            et[l, :n, c] = e
            ee[l, slot, rows, c] = e
            uu[l, i, rows, c] = val.astype(BF16)

        def down(l, c):
            g = gg[1, i, rows, c] if l == 1 else gm[:n, c]
            out = (g.astype(F32) + jnp.dot(et[l, :n], wat[l, :, c], preferred_element_type=F32)).astype(BF16)
            if l == 1:
                gm[:n, c] = out
                gg[0, i, rows, c] = out
            else:
                gout[lax.rem(i, SENDS), rows, c] = out

        steps = []
        for l in (1, 0):
            steps.append([functools.partial(up, l, c) for c in tiles(hidden)])
            steps.append([functools.partial(down, l, c) for c in tiles(model)])
        return steps

    def store_e(i):
        slot = lax.rem(i, ring)
        return pltpu.make_async_copy(ee.at[:, slot], e_hbm.at[:, i], e_out.at[slot])

    def load_e(k):
        l, first, buf = lax.rem(k // 2, 2), (k // 4) * GROUP, lax.rem(k // 2, 2)
        return pltpu.make_async_copy(e_hbm.at[l, pl.ds(first, GROUP)], es.at[buf], e_in.at[buf])

    def result(k, pick):
        l = lax.rem(k // 2, 2)
        return pltpu.make_async_copy(acc.at[pick, l], (ga_out, gb_out)[pick].at[l], o_sem.at[pick, l])

    def wgt(k, pick, direct):
        l = lax.rem(k // 2, 2)
        first = (k // 4) * GROUP
        rows = GROUP * tokens
        for r in tiles(rows):
            lo = first + r.start // tokens
            src = hh if pick == 0 else gg
            xt[:, r] = src[l, pl.ds(lo, TILE // tokens)].reshape(TILE, model).T

        def piece(c):
            if pick == 0 and direct:
                y = ee[l, pl.ds(lax.rem(first, ring), GROUP), :, c]
            elif pick == 0:
                y = es[lax.rem(k // 2, 2), :, :, c]
            else:
                y = uu[l, pl.ds(first, GROUP), :, c]
            acc[pick, l, :, c] += jnp.dot(xt[...], y.reshape(rows, TILE), preferred_element_type=F32)

        for c in tiles(hidden):
            piece(c)

    def run(*lists):
        for steps in lists:
            for pieces in steps:
                for piece in pieces:
                    piece()

    def wait_fwd(m):
        j, rows = part(m)
        pltpu.make_async_copy(hh.at[0, j, rows], hh.at[0, j, rows], f_recv.at[m]).wait()

    def wait_bwd(m):
        i, rows = part(m)

        @pl.when(is_last == False)
        def _():
            pltpu.make_async_copy(gg.at[1, i, rows], gg.at[1, i, rows], g_recv.at[m]).wait()
            send_fwd(m).wait_send()

        @pl.when((me > 0) & (m >= SENDS * HALVES))
        def _():
            send_bwd(m - SENDS * HALVES).wait_send()

    def ship_fwd(m):
        j, rows = part(m)

        @pl.when(is_last == False)
        def _():
            send_fwd(m).start()

        @pl.when(is_last)
        def _():
            pltpu.make_async_copy(gg.at[1, j, rows], gg.at[1, j, rows], g_recv.at[m]).wait()
            res = gg[0, j, rows].astype(F32) - gg[1, j, rows].astype(F32)
            gg[1, j, rows] = (res * loss_scale).astype(BF16)
            sq = jnp.sum((res * res).reshape(half // 8, 8, model), axis=0)
            total = sq[:, :128]
            for lo in range(128, model, 128):
                total = total + sq[:, lo:lo + 128]
            lossv[...] += total * (0.5 * loss_scale)

    def ship_bwd(m):
        @pl.when(me > 0)
        def _():
            send_bwd(m).start()

    def each(j, body):
        def step(b, c):
            body(j * HALVES + b)
            return c
        lax.fori_loop(0, HALVES, step, 0)

    warm = jnp.minimum(num_micro, 1 + PAIR_SLACK * ((last - me + 1) // 2) + CHIP_SLACK * ((last - me) // 2))
    near = me < NEAR
    lag = jnp.where(near, GROUP, num_micro)
    prep_at = jnp.where(me == 0, num_micro, 0)

    def slot(t, carry):
        i = t - warm
        k = i - lag
        does_f = t < num_micro
        does_b = (i >= 0) & (i < num_micro)
        does_w = k >= 0
        which = lax.rem(k + 2 * num_micro, 2)

        @pl.when(t == prep_at)
        def _():
            prepare()

        @pl.when(i == num_micro - 1)
        def _():
            @pl.when(is_last == False)
            def _():
                pltpu.make_async_copy(lossv, lossv, l_recv).wait()

            @pl.when(me > 0)
            def _():
                send_loss().start()

        @pl.when(does_f & (i < 0))
        def _():
            def step(m):
                wait_fwd(m)
                run(fwd_steps(*part(m), half))
                ship_fwd(m)
            each(t, step)

        @pl.when(does_f & (i >= 0))
        def _():
            rows = slice(None)
            each(t, wait_fwd)
            each(i, wait_bwd)
            run(fwd_steps(t, rows, tokens), bwd_steps(i, rows, tokens))
            each(i, ship_bwd)
            each(t, ship_fwd)

        @pl.when(does_b & (t >= num_micro) & near)
        def _():
            each(i, wait_bwd)
            run(bwd_steps(i, slice(None), tokens))
            each(i, ship_bwd)

        @pl.when(does_b & (t >= num_micro) & (near == False))
        def _():
            def step(m):
                wait_bwd(m)
                run(bwd_steps(*part(m), half))
                ship_bwd(m)
            each(i, step)

        @pl.when(does_b & (near == False))
        def _():
            store_e(i).start()

            @pl.when(i > 0)
            def _():
                store_e(i - 1).wait()

        @pl.when((i == num_micro) & (near == False))
        def _():
            store_e(num_micro - 1).wait()
            load_e(0).start()

        @pl.when(does_w & (which == 0) & near)
        def _():
            wgt(k, 0, True)

        @pl.when(does_w & (which == 0) & (near == False))
        def _():
            @pl.when(k + 2 < num_micro)
            def _():
                load_e(k + 2).start()
            load_e(k).wait()
            wgt(k, 0, False)

        @pl.when(does_w & (which == 1))
        def _():
            wgt(k, 1, True)

        for pick in range(2):
            @pl.when((k >= num_micro - 4) & (which == pick))
            def _(pick=pick):
                result(k, pick).start()

        return carry

    lax.fori_loop(0, num_micro + warm + lag, slot, 0)

    loss_copy = pltpu.make_async_copy(lossv, loss_out, e_in.at[0])
    loss_copy.start()

    @pl.when(me > 0)
    def _():
        send_loss().wait_send()

        def drain(m, c):
            send_bwd(m).wait_send()
            return c
        lax.fori_loop((num_micro - SENDS) * HALVES, num_micro * HALVES, drain, 0)

    loss_copy.wait()
    for k in range(4):
        result(k, k % 2).wait()


def finish(ga, gbt, loss, ga_out, gb_out, loss_out):
    ga_out[...] = ga[...]
    gb_out[0] = gbt[0].T
    loss_out[0] = jnp.sum(loss[...])


def write_results(grad_a, grad_bt, loss):
    layers, model, hidden = grad_a.shape
    rows, cols = model // 4, hidden // 4
    return pl.pallas_call(
        finish,
        grid=(layers, 4),
        in_specs=[pl.BlockSpec((1, rows, hidden), lambda l, b: (l, b, 0)), pl.BlockSpec((1, model, cols), lambda l, b: (l, 0, b)), pl.BlockSpec(loss.shape, lambda l, b: (0, 0))],
        out_specs=(pl.BlockSpec((1, rows, hidden), lambda l, b: (l, b, 0)), pl.BlockSpec((1, cols, model), lambda l, b: (l, b, 0)), pl.BlockSpec(memory_space=pltpu.SMEM)),
        out_shape=(jax.ShapeDtypeStruct((layers, model, hidden), F32), jax.ShapeDtypeStruct((layers, hidden, model), F32), jax.ShapeDtypeStruct((1,), F32)),
    )(grad_a, grad_bt, loss)


def solution(mesh):
    stages = mesh.shape['stage']

    def per_device(micro_in, targets, w_in, w_out):
        num_micro, tokens, model = micro_in.shape
        hidden = w_in.shape[-1]
        ring = min(RING, num_micro)
        any_spec = pl.BlockSpec(memory_space=pl.ANY)
        dma = pltpu.SemaphoreType.DMA
        grad_a, grad_bt, loss, _ = pl.pallas_call(
            functools.partial(kernel, stages, num_micro, ring),
            out_shape=(jax.ShapeDtypeStruct((2, model, hidden), F32), jax.ShapeDtypeStruct((2, model, hidden), F32), jax.ShapeDtypeStruct((8, 128), F32), jax.ShapeDtypeStruct((2, num_micro, tokens, hidden), BF16)),
            in_specs=[any_spec] * 4,
            out_specs=(any_spec,) * 4,
            scratch_shapes=[
                pltpu.VMEM((2, model, hidden), BF16),
                pltpu.VMEM((2, hidden, model), BF16),
                pltpu.VMEM((2, hidden, model), BF16),
                pltpu.VMEM((2, model, hidden), BF16),
                pltpu.VMEM((2, num_micro, tokens, model), BF16),
                pltpu.VMEM((2, num_micro, tokens, hidden), BF16),
                pltpu.VMEM((2, num_micro, tokens, model), BF16),
                pltpu.VMEM((2, ring, tokens, hidden), BF16),
                pltpu.VMEM((2, GROUP, tokens, hidden), BF16),
                pltpu.VMEM((2, 2, model, hidden), F32),
                pltpu.VMEM((2, tokens, hidden), BF16),
                pltpu.VMEM((2, tokens, hidden), BF16),
                pltpu.VMEM((tokens, model), BF16),
                pltpu.VMEM((tokens, model), BF16),
                pltpu.VMEM((SENDS, tokens, model), BF16),
                pltpu.VMEM((model, GROUP * tokens), BF16),
                pltpu.VMEM((8, 128), F32),
                dma((num_micro * HALVES,)), dma((num_micro * HALVES,)), dma((num_micro * HALVES,)), dma((SENDS * HALVES,)),
                dma((2,)), dma(()), dma(()), dma((2, 2)), dma((ring,)), dma((2,)),
            ],
            compiler_params=pltpu.CompilerParams(collective_id=0, has_side_effects=True, vmem_limit_bytes=67043328),
        )(micro_in, targets, w_in[0], w_out[0])
        grad_a, grad_b, total = write_results(grad_a, grad_bt, loss)
        return grad_a[None], grad_b[None], total

    return jax.shard_map(per_device, mesh=mesh, in_specs=(P('data'), P('data'), P('stage'), P('stage')), out_specs=(P(('data', 'stage')), P(('data', 'stage')), P('data')), check_vma=False)
```

```python
import functools
import jax
import jax.numpy as jnp
from jax import lax
from jax.experimental import pallas as pl
from jax.experimental.pallas import tpu as pltpu
from jax.sharding import PartitionSpec as P

BF16 = jnp.bfloat16
F32 = jnp.float32
C0 = 0.7978845608028654
C1 = 0.044715 * C0
GROUP = 4
LANES = 128
RING = 8
SENDS = 4
PAIR_SLACK = 4
CHIP_SLACK = 5
NEAR = 8
HALVES = 2
SPLIT = 2


def gelu(x):
    return x * (0.5 + 0.5 * jnp.tanh(x * (C0 + C1 * (x * x))))


def gelu_pair(x):
    sq = x * x
    t = jnp.tanh(x * (C0 + C1 * sq))
    cdf = 0.5 + 0.5 * t
    slope = cdf + (x * (0.5 * C0 + 1.5 * C1 * sq)) * (1.0 - t * t)
    return x * cdf, slope


def pairs(width):
    return [(c, c + 2) for c in range(0, width // LANES, 2)]


def join(parts):
    return jnp.concatenate(list(parts), axis=-1)


def kernel(stages, num_micro, ring, x_hbm, t_hbm, wa_hbm, wb_hbm, ga_out, gb_out, loss_out, e_hbm,
           wa, wb, wat, wbt, hh, uu, gg, ee, es, acc, act, et, hm, gm, gout, xt, lossv,
           f_recv, f_send, g_recv, g_send, w_sem, l_recv, l_send, o_sem, e_out, e_in):
    tokens = hh.shape[-2]
    model, hidden = hh.shape[-3] * LANES, uu.shape[-3] * LANES
    mcols, hcols = range(model // LANES), range(hidden // LANES)
    me = lax.axis_index('stage')
    last = stages - 1
    is_last = me == last
    loss_scale = 1.0 / (num_micro * tokens * model)

    half = tokens // HALVES

    def part(m):
        return m // HALVES, pl.ds(pl.multiple_of(lax.rem(m, HALVES) * half, half), half)

    def lanes(c):
        return pl.ds(c * LANES, LANES)

    for l in range(2):
        for c in hcols:
            pltpu.make_async_copy(wa_hbm.at[l, :, lanes(c)], wa.at[l, c], w_sem.at[0]).start()
        for c in mcols:
            pltpu.make_async_copy(wb_hbm.at[l, :, lanes(c)], wb.at[l, c], w_sem.at[1]).start()

    @pl.when(me == 0)
    def _():
        def load(m, c):
            j, rows = part(m)
            for col in mcols:
                pltpu.make_async_copy(x_hbm.at[j, rows, lanes(col)], hh.at[0, j, col, rows], f_recv.at[m]).start()
            return c
        lax.fori_loop(0, num_micro * HALVES, load, 0)

    @pl.when(is_last)
    def _():
        def load(m, c):
            j, rows = part(m)
            for col in mcols:
                pltpu.make_async_copy(t_hbm.at[j, rows, lanes(col)], gg.at[1, j, col, rows], g_recv.at[m]).start()
            return c
        lax.fori_loop(0, num_micro * HALVES, load, 0)
        lossv[...] = jnp.zeros_like(lossv)

    barrier = pltpu.get_barrier_semaphore()

    @pl.when(me > 0)
    def _():
        pl.semaphore_signal(barrier, inc=1, device_id={'stage': me - 1}, device_id_type=pl.DeviceIdType.MESH)

    @pl.when(me < last)
    def _():
        pl.semaphore_signal(barrier, inc=1, device_id={'stage': me + 1}, device_id_type=pl.DeviceIdType.MESH)

    pl.semaphore_wait(barrier, jnp.where((me == 0) | is_last, 1, 2))

    pltpu.make_async_copy(wa, wa, w_sem.at[0]).wait()
    pltpu.make_async_copy(wb, wb, w_sem.at[1]).wait()

    def send_fwd(m):
        j, rows = part(m)
        return pltpu.make_async_remote_copy(
            src_ref=gg.at[0, j, :, rows], dst_ref=hh.at[0, j, :, rows], send_sem=f_send.at[m], recv_sem=f_recv.at[m],
            device_id={'stage': jnp.minimum(me + 1, last)}, device_id_type=pl.DeviceIdType.MESH)

    def send_bwd(m):
        i, rows = part(m)
        return pltpu.make_async_remote_copy(
            src_ref=gout.at[lax.rem(i, SENDS), :, rows], dst_ref=gg.at[1, i, :, rows],
            send_sem=g_send.at[lax.rem(m, SENDS * HALVES)], recv_sem=g_recv.at[m],
            device_id={'stage': jnp.maximum(me - 1, 0)}, device_id_type=pl.DeviceIdType.MESH)

    def send_loss():
        return pltpu.make_async_remote_copy(
            src_ref=lossv, dst_ref=lossv, send_sem=l_send, recv_sem=l_recv,
            device_id={'stage': jnp.maximum(me - 1, 0)}, device_id_type=pl.DeviceIdType.MESH)

    def prepare():
        for l in range(2):
            for r in mcols:
                for c in hcols:
                    wat[l, r, lanes(c)] = wa[l, c, lanes(r)].T
                    wbt[l, c, lanes(r)] = wb[l, r, lanes(c)].T

        def clear(r, c):
            rows = pl.ds(pl.multiple_of(r * 8, 8), 8)
            for l in range(2):
                for col in hcols:
                    for which in range(2):
                        acc[which, l, col, rows] = jnp.zeros((8, LANES), F32)
            return c
        lax.fori_loop(0, model // 8, clear, 0)

    def fwd_steps(j, rows, n):
        def up(l, cols):
            h = join(hh[0, j, c, rows] if l == 0 else hm[c, :n] for c in mcols)
            pre = jnp.dot(h, join(wa[l, c] for c in range(*cols)), preferred_element_type=F32).astype(BF16)
            val = gelu(pre.astype(F32)).astype(BF16)
            for at, c in enumerate(range(*cols)):
                uu[l, j, c, rows] = pre[:, at * LANES:(at + 1) * LANES]
                act[l, c, :n] = val[:, at * LANES:(at + 1) * LANES]

        def down(l, cols):
            branch = jnp.dot(join(act[l, c, :n] for c in hcols), join(wb[l, c] for c in range(*cols)), preferred_element_type=F32)
            for at, c in enumerate(range(*cols)):
                h = hh[0, j, c, rows] if l == 0 else hm[c, :n]
                out = (h.astype(F32) + branch[:, at * LANES:(at + 1) * LANES]).astype(BF16)
                if l == 0:
                    hm[c, :n] = out
                    hh[1, j, c, rows] = out
                else:
                    gg[0, j, c, rows] = out

        steps = []
        for l in range(2):
            steps.append([functools.partial(up, l, c) for c in pairs(hidden)])
            steps.append([functools.partial(down, l, c) for c in pairs(model)])
        return steps

    def bwd_steps(i, rows, n):
        slot = lax.rem(i, ring)
        out_slot = lax.rem(i, SENDS)

        def up(l, cols):
            g = join(gg[1, i, c, rows] if l == 1 else gm[c, :n] for c in mcols)
            grad_act = jnp.dot(g, join(wbt[l, c] for c in range(*cols)), preferred_element_type=F32)
            for at, c in enumerate(range(*cols)):
                val, slope = gelu_pair(uu[l, i, c, rows].astype(F32))
                e = (slope * grad_act[:, at * LANES:(at + 1) * LANES]).astype(BF16)
                et[l, c, :n] = e
                ee[l, slot, c, rows] = e
                uu[l, i, c, rows] = val.astype(BF16)

        def down(l, cols):
            back = jnp.dot(join(et[l, c, :n] for c in hcols), join(wat[l, c] for c in range(*cols)), preferred_element_type=F32)
            for at, c in enumerate(range(*cols)):
                g = gg[1, i, c, rows] if l == 1 else gm[c, :n]
                out = (g.astype(F32) + back[:, at * LANES:(at + 1) * LANES]).astype(BF16)
                if l == 1:
                    gm[c, :n] = out
                    gg[0, i, c, rows] = out
                else:
                    gout[out_slot, c, rows] = out

        steps = []
        for l in (1, 0):
            steps.append([functools.partial(up, l, c) for c in pairs(hidden)])
            steps.append([functools.partial(down, l, c) for c in pairs(model)])
        return steps

    def store_e(i):
        slot = lax.rem(i, ring)
        return pltpu.make_async_copy(ee.at[:, slot], e_hbm.at[:, i], e_out.at[slot])

    def load_e(k):
        l, first, buf = lax.rem(k // 2, 2), (k // 4) * GROUP, lax.rem(k // 2, 2)
        return pltpu.make_async_copy(e_hbm.at[l, pl.ds(first, GROUP)], es.at[buf], e_in.at[buf])

    def result(k, pick):
        l = lax.rem(k // 2, 2)
        return pltpu.make_async_copy(acc.at[pick, l], (ga_out, gb_out)[pick].at[l], o_sem.at[pick, l])

    def wgt(k, pick, direct):
        l = lax.rem(k // 2, 2)
        first = (k // 4) * GROUP
        src = hh if pick == 0 else gg
        for q in range(GROUP):
            for c in mcols:
                xt[q, lanes(c)] = src[l, first + q, c].T

        def column(c):
            if pick == 0 and direct:
                y = ee[l, pl.ds(lax.rem(first, ring), GROUP), c]
            elif pick == 0:
                y = es[lax.rem(k // 2, 2), :, c]
            else:
                y = uu[l, pl.ds(first, GROUP), c]
            return y.reshape(GROUP * tokens, LANES)

        for cols in pairs(hidden):
            part_sum = jnp.dot(join(xt[q] for q in range(GROUP)), join(column(c) for c in range(*cols)), preferred_element_type=F32)
            for at, c in enumerate(range(*cols)):
                acc[pick, l, c] += part_sum[:, at * LANES:(at + 1) * LANES]

    def run(*lists):
        for steps in lists:
            for pieces in steps:
                for piece in pieces:
                    piece()

    def wait_fwd(m):
        j, rows = part(m)
        pltpu.make_async_copy(hh.at[0, j, :, rows], hh.at[0, j, :, rows], f_recv.at[m]).wait()

    def wait_bwd(m):
        i, rows = part(m)

        @pl.when(is_last == False)
        def _():
            pltpu.make_async_copy(gg.at[1, i, :, rows], gg.at[1, i, :, rows], g_recv.at[m]).wait()
            send_fwd(m).wait_send()

        @pl.when((me > 0) & (m >= SENDS * HALVES))
        def _():
            send_bwd(m - SENDS * HALVES).wait_send()

    def ship_fwd(m):
        j, rows = part(m)

        @pl.when(is_last == False)
        def _():
            send_fwd(m).start()

        @pl.when(is_last)
        def _():
            pltpu.make_async_copy(gg.at[1, j, :, rows], gg.at[1, j, :, rows], g_recv.at[m]).wait()
            total = jnp.zeros((8, LANES), F32)
            for c in mcols:
                res = gg[0, j, c, rows].astype(F32) - gg[1, j, c, rows].astype(F32)
                gg[1, j, c, rows] = (res * loss_scale).astype(BF16)
                total = total + jnp.sum((res * res).reshape(half // 8, 8, LANES), axis=0)
            lossv[...] += total * (0.5 * loss_scale)

    def ship_bwd(m):
        @pl.when(me > 0)
        def _():
            send_bwd(m).start()

    def each(j, body):
        def step(b, c):
            body(j * HALVES + b)
            return c
        lax.fori_loop(0, HALVES, step, 0)

    warm = jnp.minimum(num_micro, 1 + PAIR_SLACK * ((last - me + 1) // 2) + CHIP_SLACK * ((last - me) // 2))
    near = me < NEAR
    lag = jnp.where(near, GROUP, num_micro)
    prep_at = jnp.where(me == 0, num_micro, 0)

    def slot(t, carry):
        i = t - warm
        k = i - lag
        does_f = t < num_micro
        does_b = (i >= 0) & (i < num_micro)
        does_w = k >= 0
        which = lax.rem(k + 2 * num_micro, 2)

        @pl.when(t == prep_at)
        def _():
            prepare()

        @pl.when(i == num_micro - 1)
        def _():
            @pl.when(is_last == False)
            def _():
                pltpu.make_async_copy(lossv, lossv, l_recv).wait()

            @pl.when(me > 0)
            def _():
                send_loss().start()

        @pl.when(does_f & (i < 0))
        def _():
            def step(m):
                wait_fwd(m)
                run(fwd_steps(*part(m), half))
                ship_fwd(m)
            each(t, step)

        @pl.when(does_f & (i >= 0))
        def _():
            rows = slice(None)
            each(t, wait_fwd)
            each(i, wait_bwd)
            run(fwd_steps(t, rows, tokens), bwd_steps(i, rows, tokens))
            each(i, ship_bwd)
            each(t, ship_fwd)

        @pl.when(does_b & (t >= num_micro) & near)
        def _():
            each(i, wait_bwd)
            run(bwd_steps(i, slice(None), tokens))
            each(i, ship_bwd)

        @pl.when(does_b & (t >= num_micro) & (near == False))
        def _():
            def step(m):
                wait_bwd(m)
                run(bwd_steps(*part(m), half))
                ship_bwd(m)
            each(i, step)

        @pl.when(does_b & (near == False))
        def _():
            store_e(i).start()

            @pl.when(i > 0)
            def _():
                store_e(i - 1).wait()

        @pl.when((i == num_micro) & (near == False))
        def _():
            store_e(num_micro - 1).wait()
            load_e(0).start()

        @pl.when(does_w & (which == 0) & near)
        def _():
            wgt(k, 0, True)

        @pl.when(does_w & (which == 0) & (near == False))
        def _():
            @pl.when(k + 2 < num_micro)
            def _():
                load_e(k + 2).start()
            load_e(k).wait()
            wgt(k, 0, False)

        @pl.when(does_w & (which == 1))
        def _():
            wgt(k, 1, True)

        for pick in range(2):
            @pl.when((k >= num_micro - 4) & (which == pick))
            def _(pick=pick):
                result(k, pick).start()

        return carry

    lax.fori_loop(0, num_micro + warm + lag, slot, 0)

    loss_copy = pltpu.make_async_copy(lossv, loss_out, e_in.at[0])
    loss_copy.start()

    @pl.when(me > 0)
    def _():
        send_loss().wait_send()

        def drain(m, c):
            send_bwd(m).wait_send()
            return c
        lax.fori_loop((num_micro - SENDS) * HALVES, num_micro * HALVES, drain, 0)

    loss_copy.wait()
    for k in range(4):
        result(k, k % 2).wait()


def finish(ga, gbt, loss, ga_out, gb_out, loss_out):
    for c in range(ga.shape[1]):
        ga_out[0, :, c * LANES:(c + 1) * LANES] = ga[0, c]
    for c in range(gbt.shape[1]):
        gb_out[0, c * LANES:(c + 1) * LANES] = gbt[0, c].T
    loss_out[0] = jnp.sum(loss[...])


def write_results(grad_a, grad_bt, loss):
    layers, cols, model, _ = grad_a.shape
    hidden = cols * LANES
    rows = model // SPLIT
    return pl.pallas_call(
        finish,
        grid=(layers, SPLIT),
        in_specs=[pl.BlockSpec((1, cols, rows, LANES), lambda l, b: (l, 0, b, 0)), pl.BlockSpec((1, cols // SPLIT, model, LANES), lambda l, b: (l, b, 0, 0)), pl.BlockSpec(loss.shape, lambda l, b: (0, 0))],
        out_specs=(pl.BlockSpec((1, rows, hidden), lambda l, b: (l, b, 0)), pl.BlockSpec((1, hidden // SPLIT, model), lambda l, b: (l, b, 0)), pl.BlockSpec(memory_space=pltpu.SMEM)),
        out_shape=(jax.ShapeDtypeStruct((layers, model, hidden), F32), jax.ShapeDtypeStruct((layers, hidden, model), F32), jax.ShapeDtypeStruct((1,), F32)),
    )(grad_a, grad_bt, loss)


def solution(mesh):
    stages = mesh.shape['stage']

    def per_device(micro_in, targets, w_in, w_out):
        num_micro, tokens, model = micro_in.shape
        hidden = w_in.shape[-1]
        ring = min(RING, num_micro)
        any_spec = pl.BlockSpec(memory_space=pl.ANY)
        dma = pltpu.SemaphoreType.DMA
        mcols, hcols = model // LANES, hidden // LANES
        grad = jax.ShapeDtypeStruct((2, hcols, model, LANES), F32)
        grad_a, grad_bt, loss, _ = pl.pallas_call(
            functools.partial(kernel, stages, num_micro, ring),
            out_shape=(grad, grad, jax.ShapeDtypeStruct((8, 128), F32), jax.ShapeDtypeStruct((2, num_micro, hcols, tokens, LANES), BF16)),
            in_specs=[any_spec] * 4,
            out_specs=(any_spec,) * 4,
            scratch_shapes=[
                pltpu.VMEM((2, hcols, model, LANES), BF16),
                pltpu.VMEM((2, mcols, hidden, LANES), BF16),
                pltpu.VMEM((2, mcols, hidden, LANES), BF16),
                pltpu.VMEM((2, hcols, model, LANES), BF16),
                pltpu.VMEM((2, num_micro, mcols, tokens, LANES), BF16),
                pltpu.VMEM((2, num_micro, hcols, tokens, LANES), BF16),
                pltpu.VMEM((2, num_micro, mcols, tokens, LANES), BF16),
                pltpu.VMEM((2, ring, hcols, tokens, LANES), BF16),
                pltpu.VMEM((2, GROUP, hcols, tokens, LANES), BF16),
                pltpu.VMEM((2, 2, hcols, model, LANES), F32),
                pltpu.VMEM((2, hcols, tokens, LANES), BF16),
                pltpu.VMEM((2, hcols, tokens, LANES), BF16),
                pltpu.VMEM((mcols, tokens, LANES), BF16),
                pltpu.VMEM((mcols, tokens, LANES), BF16),
                pltpu.VMEM((SENDS, mcols, tokens, LANES), BF16),
                pltpu.VMEM((GROUP * tokens // LANES, model, LANES), BF16),
                pltpu.VMEM((8, 128), F32),
                dma((num_micro * HALVES,)), dma((num_micro * HALVES,)), dma((num_micro * HALVES,)), dma((SENDS * HALVES,)),
                dma((2,)), dma(()), dma(()), dma((2, 2)), dma((ring,)), dma((2,)),
            ],
            compiler_params=pltpu.CompilerParams(collective_id=0, has_side_effects=True, vmem_limit_bytes=67043328),
        )(micro_in, targets, w_in[0], w_out[0])
        grad_a, grad_b, total = write_results(grad_a, grad_bt, loss)
        return grad_a[None], grad_b[None], total

    return jax.shard_map(per_device, mesh=mesh, in_specs=(P('data'), P('data'), P('stage'), P('stage')), out_specs=(P(('data', 'stage')), P(('data', 'stage')), P('data')), check_vma=False)
```

```python
import functools
import jax
import jax.numpy as jnp
from jax import lax
from jax.experimental import pallas as pl
from jax.experimental.pallas import tpu as pltpu
from jax.sharding import PartitionSpec as P

BF16 = jnp.bfloat16
F32 = jnp.float32
C0 = 0.7978845608028654
C1 = 0.044715 * C0
GROUP = 4
TILE = 256
RING = 8
SENDS = 4
PAIR_SLACK = 2
CHIP_SLACK = 5
NEAR = 8
HALVES = 2
LATE = 4
SPLIT = 2


def gelu(x):
    return x * (0.5 + 0.5 * jnp.tanh(x * (C0 + C1 * (x * x))))


def gelu_pair(x):
    sq = x * x
    t = jnp.tanh(x * (C0 + C1 * sq))
    cdf = 0.5 + 0.5 * t
    slope = cdf + (x * (0.5 * C0 + 1.5 * C1 * sq)) * (1.0 - t * t)
    return x * cdf, slope


def tiles(width):
    return [slice(lo, lo + TILE) for lo in range(0, width, TILE)]


def kernel(stages, num_micro, ring, x_hbm, t_hbm, wa_hbm, wb_hbm, ga_out, gb_out, loss_out, e_hbm,
           wa, wb, wat, wbt, hh, uu, gg, ee, es, acc, act, et, hm, gm, gout, xt, lossv,
           f_recv, f_send, g_recv, g_send, w_sem, l_recv, l_send, o_sem, e_out, e_in):
    tokens, model = hh.shape[-2:]
    hidden = uu.shape[-1]
    me = lax.axis_index('stage')
    last = stages - 1
    is_last = me == last
    loss_scale = 1.0 / (num_micro * tokens * model)

    half = tokens // HALVES

    def part(m):
        return m // HALVES, pl.ds(pl.multiple_of(lax.rem(m, HALVES) * half, half), half)

    def weight_copies():
        return (pltpu.make_async_copy(wa_hbm, wa, w_sem.at[0]), pltpu.make_async_copy(wb_hbm, wb, w_sem.at[1]))

    for copy in weight_copies():
        copy.start()

    @pl.when(me == 0)
    def _():
        def load(m, c):
            j, rows = part(m)
            pltpu.make_async_copy(x_hbm.at[j, rows], hh.at[0, j, rows], f_recv.at[m]).start()
            return c
        lax.fori_loop(0, num_micro * HALVES, load, 0)

    @pl.when(is_last)
    def _():
        def load(m, c):
            j, rows = part(m)
            pltpu.make_async_copy(t_hbm.at[j, rows], gg.at[1, j, rows], g_recv.at[m]).start()
            return c
        lax.fori_loop(0, num_micro * HALVES, load, 0)
        lossv[...] = jnp.zeros_like(lossv)

    barrier = pltpu.get_barrier_semaphore()

    @pl.when(me > 0)
    def _():
        pl.semaphore_signal(barrier, inc=1, device_id={'stage': me - 1}, device_id_type=pl.DeviceIdType.MESH)

    @pl.when(me < last)
    def _():
        pl.semaphore_signal(barrier, inc=1, device_id={'stage': me + 1}, device_id_type=pl.DeviceIdType.MESH)

    pl.semaphore_wait(barrier, jnp.where((me == 0) | is_last, 1, 2))

    for copy in weight_copies():
        copy.wait()

    def send_fwd(m):
        j, rows = part(m)
        return pltpu.make_async_remote_copy(
            src_ref=gg.at[0, j, rows], dst_ref=hh.at[0, j, rows], send_sem=f_send.at[m], recv_sem=f_recv.at[m],
            device_id={'stage': jnp.minimum(me + 1, last)}, device_id_type=pl.DeviceIdType.MESH)

    def send_bwd(m):
        i, rows = part(m)
        return pltpu.make_async_remote_copy(
            src_ref=gout.at[lax.rem(i, SENDS), rows], dst_ref=gg.at[1, i, rows],
            send_sem=g_send.at[lax.rem(m, SENDS * HALVES)], recv_sem=g_recv.at[m],
            device_id={'stage': jnp.maximum(me - 1, 0)}, device_id_type=pl.DeviceIdType.MESH)

    def send_loss():
        return pltpu.make_async_remote_copy(
            src_ref=lossv, dst_ref=lossv, send_sem=l_send, recv_sem=l_recv,
            device_id={'stage': jnp.maximum(me - 1, 0)}, device_id_type=pl.DeviceIdType.MESH)

    def prepare():
        for l in range(2):
            for r in tiles(model):
                for c in tiles(hidden):
                    wat[l, c, r] = wa[l, r, c].T
                    wbt[l, r, c] = wb[l, c, r].T

        def clear(r, c):
            acc[r // (2 * model // 8), lax.rem(r // (model // 8), 2), pl.ds(lax.rem(r, model // 8) * 8, 8), :] = jnp.zeros((8, hidden), F32)
            return c
        lax.fori_loop(0, 4 * model // 8, clear, 0)

    def fwd_steps(j, rows, n):
        def up(l, c):
            h = hh[0, j, rows] if l == 0 else hm[:n]
            pre = jnp.dot(h, wa[l, :, c], preferred_element_type=F32).astype(BF16)
            uu[l, j, rows, c] = pre
            act[l, :n, c] = gelu(pre.astype(F32)).astype(BF16)

        def down(l, c):
            h = hh[0, j, rows, c] if l == 0 else hm[:n, c]
            out = (h.astype(F32) + jnp.dot(act[l, :n], wb[l, :, c], preferred_element_type=F32)).astype(BF16)
            if l == 0:
                hm[:n, c] = out
                hh[1, j, rows, c] = out
            else:
                gg[0, j, rows, c] = out

        steps = []
        for l in range(2):
            steps.append([functools.partial(up, l, c) for c in tiles(hidden)])
            steps.append([functools.partial(down, l, c) for c in tiles(model)])
        return steps

    def bwd_steps(i, rows, n):
        slot = lax.rem(i, ring)

        def up(l, c):
            g = gg[1, i, rows] if l == 1 else gm[:n]
            grad_act = jnp.dot(g, wbt[l, :, c], preferred_element_type=F32)
            val, slope = gelu_pair(uu[l, i, rows, c].astype(F32))
            e = (slope * grad_act).astype(BF16)
            et[l, :n, c] = e
            ee[l, slot, rows, c] = e
            uu[l, i, rows, c] = val.astype(BF16)

        def down(l, c):
            g = gg[1, i, rows, c] if l == 1 else gm[:n, c]
            out = (g.astype(F32) + jnp.dot(et[l, :n], wat[l, :, c], preferred_element_type=F32)).astype(BF16)
            if l == 1:
                gm[:n, c] = out
                gg[0, i, rows, c] = out
            else:
                gout[lax.rem(i, SENDS), rows, c] = out

        steps = []
        for l in (1, 0):
            steps.append([functools.partial(up, l, c) for c in tiles(hidden)])
            steps.append([functools.partial(down, l, c) for c in tiles(model)])
        return steps

    def store_e(i):
        slot = lax.rem(i, ring)
        return pltpu.make_async_copy(ee.at[:, slot], e_hbm.at[:, i], e_out.at[slot])

    def load_e(k):
        l, first, buf = lax.rem(k // 2, 2), (k // 4) * GROUP, lax.rem(k // 2, 2)
        return pltpu.make_async_copy(e_hbm.at[l, pl.ds(first, GROUP)], es.at[buf], e_in.at[buf])

    def result(k, pick):
        l = lax.rem(k // 2, 2)
        return pltpu.make_async_copy(acc.at[pick, l], (ga_out, gb_out)[pick].at[l], o_sem.at[pick, l])

    def wgt(k, pick, direct):
        l = lax.rem(k // 2, 2)
        first = (k // 4) * GROUP
        rows = GROUP * tokens
        for r in tiles(rows):
            lo = first + r.start // tokens
            src = hh if pick == 0 else gg
            xt[:, r] = src[l, pl.ds(lo, TILE // tokens)].reshape(TILE, model).T

        def piece(c):
            if pick == 0 and direct:
                y = ee[l, pl.ds(lax.rem(first, ring), GROUP), :, c]
            elif pick == 0:
                y = es[lax.rem(k // 2, 2), :, :, c]
            else:
                y = uu[l, pl.ds(first, GROUP), :, c]
            acc[pick, l, :, c] += jnp.dot(xt[...], y.reshape(rows, TILE), preferred_element_type=F32)

        for c in tiles(hidden):
            piece(c)

    def run(*lists):
        for steps in lists:
            for pieces in steps:
                for piece in pieces:
                    piece()

    def wait_fwd(m):
        j, rows = part(m)
        pltpu.make_async_copy(hh.at[0, j, rows], hh.at[0, j, rows], f_recv.at[m]).wait()

    def wait_bwd(m):
        i, rows = part(m)

        @pl.when(is_last == False)
        def _():
            pltpu.make_async_copy(gg.at[1, i, rows], gg.at[1, i, rows], g_recv.at[m]).wait()
            send_fwd(m).wait_send()

        @pl.when((me > 0) & (m >= SENDS * HALVES))
        def _():
            send_bwd(m - SENDS * HALVES).wait_send()

    def ship_fwd(m):
        j, rows = part(m)

        @pl.when(is_last == False)
        def _():
            send_fwd(m).start()

        @pl.when(is_last)
        def _():
            pltpu.make_async_copy(gg.at[1, j, rows], gg.at[1, j, rows], g_recv.at[m]).wait()
            res = gg[0, j, rows].astype(F32) - gg[1, j, rows].astype(F32)
            gg[1, j, rows] = (res * loss_scale).astype(BF16)
            sq = jnp.sum((res * res).reshape(half // 8, 8, model), axis=0)
            total = sq[:, :128]
            for lo in range(128, model, 128):
                total = total + sq[:, lo:lo + 128]
            lossv[...] += total * (0.5 * loss_scale)

    def ship_bwd(m):
        @pl.when(me > 0)
        def _():
            send_bwd(m).start()

    def each(j, body):
        def step(b, c):
            body(j * HALVES + b)
            return c
        lax.fori_loop(0, HALVES, step, 0)

    warm = jnp.minimum(num_micro, PAIR_SLACK * ((last - me + 1) // 2) + CHIP_SLACK * ((last - me) // 2))
    near = me < NEAR
    lag = jnp.where(near, GROUP, num_micro)
    prep_at = jnp.where(me == 0, num_micro, 0)

    def slot(t, carry):
        i = t - warm
        k = i - lag
        does_f = t < num_micro
        does_b = (i >= 0) & (i < num_micro)
        does_w = k >= 0
        which = lax.rem(k + 2 * num_micro, 2)

        @pl.when(t == prep_at)
        def _():
            prepare()

        f_split = (i < 0) & (me < stages - LATE)
        b_split = (t >= num_micro) & (near == False) & (me < stages - LATE)
        whole = slice(None)

        @pl.when(does_f & f_split)
        def _():
            def step(m):
                wait_fwd(m)
                run(fwd_steps(*part(m), half))
                ship_fwd(m)
            each(t, step)

        @pl.when(does_f & (f_split == False))
        def _():
            each(t, wait_fwd)
            run(fwd_steps(t, whole, tokens))
            each(t, ship_fwd)

        @pl.when(i == num_micro - 1)
        def _():
            @pl.when(is_last == False)
            def _():
                pltpu.make_async_copy(lossv, lossv, l_recv).wait()

            @pl.when(me > 0)
            def _():
                send_loss().start()

        @pl.when(does_b & b_split)
        def _():
            def step(m):
                wait_bwd(m)
                run(bwd_steps(*part(m), half))
                ship_bwd(m)
            each(i, step)

        @pl.when(does_b & (b_split == False))
        def _():
            each(i, wait_bwd)
            run(bwd_steps(i, whole, tokens))
            each(i, ship_bwd)

        @pl.when(does_b & (near == False))
        def _():
            store_e(i).start()

            @pl.when(i > 0)
            def _():
                store_e(i - 1).wait()

        @pl.when((i == num_micro) & (near == False))
        def _():
            store_e(num_micro - 1).wait()
            load_e(0).start()

        @pl.when(does_w & (which == 0) & near)
        def _():
            wgt(k, 0, True)

        @pl.when(does_w & (which == 0) & (near == False))
        def _():
            @pl.when(k + 2 < num_micro)
            def _():
                load_e(k + 2).start()
            load_e(k).wait()
            wgt(k, 0, False)

        @pl.when(does_w & (which == 1))
        def _():
            wgt(k, 1, True)

        for pick in range(2):
            @pl.when((k >= num_micro - 4) & (which == pick))
            def _(pick=pick):
                result(k, pick).start()

        return carry

    lax.fori_loop(0, num_micro + warm + lag, slot, 0)

    loss_copy = pltpu.make_async_copy(lossv, loss_out, e_in.at[0])
    loss_copy.start()

    @pl.when(me > 0)
    def _():
        send_loss().wait_send()

        def drain(m, c):
            send_bwd(m).wait_send()
            return c
        lax.fori_loop((num_micro - SENDS) * HALVES, num_micro * HALVES, drain, 0)

    loss_copy.wait()
    for k in range(4):
        result(k, k % 2).wait()


def finish(ga, gbt, loss, ga_out, gb_out, loss_out):
    ga_out[...] = ga[...]
    gb_out[0] = gbt[0].T
    loss_out[0] = jnp.sum(loss[...])


def write_results(grad_a, grad_bt, loss):
    layers, model, hidden = grad_a.shape
    rows, cols = model // SPLIT, hidden // SPLIT
    return pl.pallas_call(
        finish,
        grid=(layers, SPLIT),
        in_specs=[pl.BlockSpec((1, rows, hidden), lambda l, b: (l, b, 0)), pl.BlockSpec((1, model, cols), lambda l, b: (l, 0, b)), pl.BlockSpec(loss.shape, lambda l, b: (0, 0))],
        out_specs=(pl.BlockSpec((1, rows, hidden), lambda l, b: (l, b, 0)), pl.BlockSpec((1, cols, model), lambda l, b: (l, b, 0)), pl.BlockSpec(memory_space=pltpu.SMEM)),
        out_shape=(jax.ShapeDtypeStruct((layers, model, hidden), F32), jax.ShapeDtypeStruct((layers, hidden, model), F32), jax.ShapeDtypeStruct((1,), F32)),
    )(grad_a, grad_bt, loss)


def solution(mesh):
    stages = mesh.shape['stage']

    def per_device(micro_in, targets, w_in, w_out):
        num_micro, tokens, model = micro_in.shape
        hidden = w_in.shape[-1]
        ring = min(RING, num_micro)
        any_spec = pl.BlockSpec(memory_space=pl.ANY)
        dma = pltpu.SemaphoreType.DMA
        grad_a, grad_bt, loss, _ = pl.pallas_call(
            functools.partial(kernel, stages, num_micro, ring),
            out_shape=(jax.ShapeDtypeStruct((2, model, hidden), F32), jax.ShapeDtypeStruct((2, model, hidden), F32), jax.ShapeDtypeStruct((8, 128), F32), jax.ShapeDtypeStruct((2, num_micro, tokens, hidden), BF16)),
            in_specs=[any_spec] * 4,
            out_specs=(any_spec,) * 4,
            scratch_shapes=[
                pltpu.VMEM((2, model, hidden), BF16),
                pltpu.VMEM((2, hidden, model), BF16),
                pltpu.VMEM((2, hidden, model), BF16),
                pltpu.VMEM((2, model, hidden), BF16),
                pltpu.VMEM((2, num_micro, tokens, model), BF16),
                pltpu.VMEM((2, num_micro, tokens, hidden), BF16),
                pltpu.VMEM((2, num_micro, tokens, model), BF16),
                pltpu.VMEM((2, ring, tokens, hidden), BF16),
                pltpu.VMEM((2, GROUP, tokens, hidden), BF16),
                pltpu.VMEM((2, 2, model, hidden), F32),
                pltpu.VMEM((2, tokens, hidden), BF16),
                pltpu.VMEM((2, tokens, hidden), BF16),
                pltpu.VMEM((tokens, model), BF16),
                pltpu.VMEM((tokens, model), BF16),
                pltpu.VMEM((SENDS, tokens, model), BF16),
                pltpu.VMEM((model, GROUP * tokens), BF16),
                pltpu.VMEM((8, 128), F32),
                dma((num_micro * HALVES,)), dma((num_micro * HALVES,)), dma((num_micro * HALVES,)), dma((SENDS * HALVES,)),
                dma((2,)), dma(()), dma(()), dma((2, 2)), dma((ring,)), dma((2,)),
            ],
            compiler_params=pltpu.CompilerParams(collective_id=0, has_side_effects=True, vmem_limit_bytes=67043328),
        )(micro_in, targets, w_in[0], w_out[0])
        grad_a, grad_b, total = write_results(grad_a, grad_bt, loss)
        return grad_a[None], grad_b[None], total

    return jax.shard_map(per_device, mesh=mesh, in_specs=(P('data'), P('data'), P('stage'), P('stage')), out_specs=(P(('data', 'stage')), P(('data', 'stage')), P('data')), check_vma=False)
```

```python
import functools
import jax
import jax.numpy as jnp
from jax import lax
from jax.experimental import pallas as pl
from jax.experimental.pallas import tpu as pltpu
from jax.sharding import PartitionSpec as P

BF16 = jnp.bfloat16
F32 = jnp.float32
C0 = 0.7978845608028654
C1 = 0.044715 * C0
GROUP = 4
TILE = 256
RING = 8
SENDS = 4
PAIR_SLACK = 2
CHIP_SLACK = 5
NEAR = 7
HALVES = 2
LATE = 4
SPLIT = 2


def gelu(x):
    return x * (0.5 + 0.5 * jnp.tanh(x * (C0 + C1 * (x * x))))


def gelu_pair(x):
    sq = x * x
    t = jnp.tanh(x * (C0 + C1 * sq))
    cdf = 0.5 + 0.5 * t
    slope = cdf + (x * (0.5 * C0 + 1.5 * C1 * sq)) * (1.0 - t * t)
    return x * cdf, slope


def tiles(width):
    return [slice(lo, lo + TILE) for lo in range(0, width, TILE)]


def kernel(stages, num_micro, ring, x_hbm, t_hbm, wa_hbm, wb_hbm, ga_out, gb_out, loss_out, e_hbm,
           wa, wb, wat, wbt, hh, uu, gg, ee, es, acc, act, et, hm, gm, gout, xt, lossv,
           f_recv, f_send, g_recv, g_send, w_sem, l_recv, l_send, o_sem, e_out, e_in):
    tokens, model = hh.shape[-2:]
    hidden = uu.shape[-1]
    me = lax.axis_index('stage')
    last = stages - 1
    is_last = me == last
    loss_scale = 1.0 / (num_micro * tokens * model)

    half = tokens // HALVES

    def part(m):
        return m // HALVES, pl.ds(pl.multiple_of(lax.rem(m, HALVES) * half, half), half)

    def weight_copies():
        return (pltpu.make_async_copy(wa_hbm, wa, w_sem.at[0]), pltpu.make_async_copy(wb_hbm, wb, w_sem.at[1]))

    for copy in weight_copies():
        copy.start()

    @pl.when(me == 0)
    def _():
        def load(m, c):
            j, rows = part(m)
            pltpu.make_async_copy(x_hbm.at[j, rows], hh.at[0, j, rows], f_recv.at[m]).start()
            return c
        lax.fori_loop(0, num_micro * HALVES, load, 0)

    @pl.when(is_last)
    def _():
        def load(m, c):
            j, rows = part(m)
            pltpu.make_async_copy(t_hbm.at[j, rows], gg.at[1, j, rows], g_recv.at[m]).start()
            return c
        lax.fori_loop(0, num_micro * HALVES, load, 0)
        lossv[...] = jnp.zeros_like(lossv)

    barrier = pltpu.get_barrier_semaphore()

    @pl.when(me > 0)
    def _():
        pl.semaphore_signal(barrier, inc=1, device_id={'stage': me - 1}, device_id_type=pl.DeviceIdType.MESH)

    @pl.when(me < last)
    def _():
        pl.semaphore_signal(barrier, inc=1, device_id={'stage': me + 1}, device_id_type=pl.DeviceIdType.MESH)

    pl.semaphore_wait(barrier, jnp.where((me == 0) | is_last, 1, 2))

    for copy in weight_copies():
        copy.wait()

    def send_fwd(m):
        j, rows = part(m)
        return pltpu.make_async_remote_copy(
            src_ref=gg.at[0, j, rows], dst_ref=hh.at[0, j, rows], send_sem=f_send.at[m], recv_sem=f_recv.at[m],
            device_id={'stage': jnp.minimum(me + 1, last)}, device_id_type=pl.DeviceIdType.MESH)

    def send_bwd(m):
        i, rows = part(m)
        return pltpu.make_async_remote_copy(
            src_ref=gout.at[lax.rem(i, SENDS), rows], dst_ref=gg.at[1, i, rows],
            send_sem=g_send.at[lax.rem(m, SENDS * HALVES)], recv_sem=g_recv.at[m],
            device_id={'stage': jnp.maximum(me - 1, 0)}, device_id_type=pl.DeviceIdType.MESH)

    def send_loss():
        return pltpu.make_async_remote_copy(
            src_ref=lossv, dst_ref=lossv, send_sem=l_send, recv_sem=l_recv,
            device_id={'stage': jnp.maximum(me - 1, 0)}, device_id_type=pl.DeviceIdType.MESH)

    def prepare():
        for l in range(2):
            for r in tiles(model):
                for c in tiles(hidden):
                    wat[l, c, r] = wa[l, r, c].T
                    wbt[l, r, c] = wb[l, c, r].T

        def clear(r, c):
            acc[r // (2 * model // 8), lax.rem(r // (model // 8), 2), pl.ds(lax.rem(r, model // 8) * 8, 8), :] = jnp.zeros((8, hidden), F32)
            return c
        lax.fori_loop(0, 4 * model // 8, clear, 0)

    def fwd_steps(j, rows, n):
        def up(l, c):
            h = hh[0, j, rows] if l == 0 else hm[:n]
            pre = jnp.dot(h, wa[l, :, c], preferred_element_type=F32).astype(BF16)
            uu[l, j, rows, c] = pre
            act[l, :n, c] = gelu(pre.astype(F32)).astype(BF16)

        def down(l, c):
            h = hh[0, j, rows, c] if l == 0 else hm[:n, c]
            out = (h.astype(F32) + jnp.dot(act[l, :n], wb[l, :, c], preferred_element_type=F32)).astype(BF16)
            if l == 0:
                hm[:n, c] = out
                hh[1, j, rows, c] = out
            else:
                gg[0, j, rows, c] = out

        steps = []
        for l in range(2):
            steps.append([functools.partial(up, l, c) for c in tiles(hidden)])
            steps.append([functools.partial(down, l, c) for c in tiles(model)])
        return steps

    def bwd_steps(i, rows, n):
        slot = lax.rem(i, ring)

        def up(l, c):
            g = gg[1, i, rows] if l == 1 else gm[:n]
            grad_act = jnp.dot(g, wbt[l, :, c], preferred_element_type=F32)
            val, slope = gelu_pair(uu[l, i, rows, c].astype(F32))
            e = (slope * grad_act).astype(BF16)
            et[l, :n, c] = e
            ee[l, slot, rows, c] = e
            uu[l, i, rows, c] = val.astype(BF16)

        def down(l, c):
            g = gg[1, i, rows, c] if l == 1 else gm[:n, c]
            out = (g.astype(F32) + jnp.dot(et[l, :n], wat[l, :, c], preferred_element_type=F32)).astype(BF16)
            if l == 1:
                gm[:n, c] = out
                gg[0, i, rows, c] = out
            else:
                gout[lax.rem(i, SENDS), rows, c] = out

        steps = []
        for l in (1, 0):
            steps.append([functools.partial(up, l, c) for c in tiles(hidden)])
            steps.append([functools.partial(down, l, c) for c in tiles(model)])
        return steps

    def store_e(i):
        slot = lax.rem(i, ring)
        return pltpu.make_async_copy(ee.at[:, slot], e_hbm.at[:, i], e_out.at[slot])

    def load_e(k):
        l, first, buf = lax.rem(k // 2, 2), (k // 4) * GROUP, lax.rem(k // 2, 2)
        return pltpu.make_async_copy(e_hbm.at[l, pl.ds(first, GROUP)], es.at[buf], e_in.at[buf])

    def result(k, pick):
        l = lax.rem(k // 2, 2)
        return pltpu.make_async_copy(acc.at[pick, l], (ga_out, gb_out)[pick].at[l], o_sem.at[pick, l])

    def wgt(k, pick, direct):
        l = lax.rem(k // 2, 2)
        first = (k // 4) * GROUP
        rows = GROUP * tokens
        for r in tiles(rows):
            lo = first + r.start // tokens
            src = hh if pick == 0 else gg
            xt[:, r] = src[l, pl.ds(lo, TILE // tokens)].reshape(TILE, model).T

        def piece(c):
            if pick == 0 and direct:
                y = ee[l, pl.ds(lax.rem(first, ring), GROUP), :, c]
            elif pick == 0:
                y = es[lax.rem(k // 2, 2), :, :, c]
            else:
                y = uu[l, pl.ds(first, GROUP), :, c]
            acc[pick, l, :, c] += jnp.dot(xt[...], y.reshape(rows, TILE), preferred_element_type=F32)

        for c in tiles(hidden):
            piece(c)

    def run(*lists):
        for steps in lists:
            for pieces in steps:
                for piece in pieces:
                    piece()

    def wait_fwd(m):
        j, rows = part(m)
        pltpu.make_async_copy(hh.at[0, j, rows], hh.at[0, j, rows], f_recv.at[m]).wait()

    def wait_bwd(m):
        i, rows = part(m)

        @pl.when(is_last == False)
        def _():
            pltpu.make_async_copy(gg.at[1, i, rows], gg.at[1, i, rows], g_recv.at[m]).wait()
            send_fwd(m).wait_send()

        @pl.when((me > 0) & (m >= SENDS * HALVES))
        def _():
            send_bwd(m - SENDS * HALVES).wait_send()

    def ship_fwd(m):
        j, rows = part(m)

        @pl.when(is_last == False)
        def _():
            send_fwd(m).start()

        @pl.when(is_last)
        def _():
            pltpu.make_async_copy(gg.at[1, j, rows], gg.at[1, j, rows], g_recv.at[m]).wait()
            res = gg[0, j, rows].astype(F32) - gg[1, j, rows].astype(F32)
            gg[1, j, rows] = (res * loss_scale).astype(BF16)
            sq = jnp.sum((res * res).reshape(half // 8, 8, model), axis=0)
            total = sq[:, :128]
            for lo in range(128, model, 128):
                total = total + sq[:, lo:lo + 128]
            lossv[...] += total * (0.5 * loss_scale)

    def ship_bwd(m):
        @pl.when(me > 0)
        def _():
            send_bwd(m).start()

    def each(j, body):
        def step(b, c):
            body(j * HALVES + b)
            return c
        lax.fori_loop(0, HALVES, step, 0)

    warm = jnp.minimum(num_micro, PAIR_SLACK * ((last - me + 1) // 2) + CHIP_SLACK * ((last - me) // 2))
    near = me < NEAR
    lag = jnp.where(near, GROUP, num_micro)
    prep_at = jnp.where(me == 0, num_micro, 0)

    def slot(t, carry):
        i = t - warm
        k = i - lag
        does_f = t < num_micro
        does_b = (i >= 0) & (i < num_micro)
        does_w = k >= 0
        which = lax.rem(k + 2 * num_micro, 2)

        @pl.when(t == prep_at)
        def _():
            prepare()

        f_split = (i < 0) & (me < stages - LATE)
        b_split = (t >= num_micro) & (near == False) & (me < stages - LATE)
        whole = slice(None)

        @pl.when(does_f & f_split)
        def _():
            def step(m):
                wait_fwd(m)
                run(fwd_steps(*part(m), half))
                ship_fwd(m)
            each(t, step)

        @pl.when(does_f & (f_split == False))
        def _():
            each(t, wait_fwd)
            run(fwd_steps(t, whole, tokens))
            each(t, ship_fwd)

        @pl.when((i == num_micro) & (near == False))
        def _():
            store_e(num_micro - 1).wait()
            load_e(0).start()

        @pl.when(does_w & (which == 0) & near)
        def _():
            wgt(k, 0, True)

        @pl.when(does_w & (which == 0) & (near == False))
        def _():
            @pl.when(k + 2 < num_micro)
            def _():
                load_e(k + 2).start()
            load_e(k).wait()
            wgt(k, 0, False)

        @pl.when(does_w & (which == 1))
        def _():
            wgt(k, 1, True)

        for pick in range(2):
            @pl.when((k >= num_micro - 4) & (which == pick))
            def _(pick=pick):
                result(k, pick).start()

        @pl.when(i == num_micro - 1)
        def _():
            @pl.when(is_last == False)
            def _():
                pltpu.make_async_copy(lossv, lossv, l_recv).wait()

            @pl.when(me > 0)
            def _():
                send_loss().start()

        @pl.when(does_b & b_split)
        def _():
            def step(m):
                wait_bwd(m)
                run(bwd_steps(*part(m), half))
                ship_bwd(m)
            each(i, step)

        @pl.when(does_b & (b_split == False))
        def _():
            each(i, wait_bwd)
            run(bwd_steps(i, whole, tokens))
            each(i, ship_bwd)

        @pl.when(does_b & (near == False))
        def _():
            store_e(i).start()

            @pl.when(i > 0)
            def _():
                store_e(i - 1).wait()

        return carry

    lax.fori_loop(0, num_micro + warm + lag, slot, 0)

    loss_copy = pltpu.make_async_copy(lossv, loss_out, e_in.at[0])
    loss_copy.start()

    @pl.when(me > 0)
    def _():
        send_loss().wait_send()

        def drain(m, c):
            send_bwd(m).wait_send()
            return c
        lax.fori_loop((num_micro - SENDS) * HALVES, num_micro * HALVES, drain, 0)

    loss_copy.wait()
    for k in range(4):
        result(k, k % 2).wait()


def finish(ga, gbt, loss, ga_out, gb_out, loss_out):
    ga_out[...] = ga[...]
    gb_out[0] = gbt[0].T
    loss_out[0] = jnp.sum(loss[...])


def write_results(grad_a, grad_bt, loss):
    layers, model, hidden = grad_a.shape
    rows, cols = model // SPLIT, hidden // SPLIT
    return pl.pallas_call(
        finish,
        grid=(layers, SPLIT),
        in_specs=[pl.BlockSpec((1, rows, hidden), lambda l, b: (l, b, 0)), pl.BlockSpec((1, model, cols), lambda l, b: (l, 0, b)), pl.BlockSpec(loss.shape, lambda l, b: (0, 0))],
        out_specs=(pl.BlockSpec((1, rows, hidden), lambda l, b: (l, b, 0)), pl.BlockSpec((1, cols, model), lambda l, b: (l, b, 0)), pl.BlockSpec(memory_space=pltpu.SMEM)),
        out_shape=(jax.ShapeDtypeStruct((layers, model, hidden), F32), jax.ShapeDtypeStruct((layers, hidden, model), F32), jax.ShapeDtypeStruct((1,), F32)),
    )(grad_a, grad_bt, loss)


def solution(mesh):
    stages = mesh.shape['stage']

    def per_device(micro_in, targets, w_in, w_out):
        num_micro, tokens, model = micro_in.shape
        hidden = w_in.shape[-1]
        ring = min(RING, num_micro)
        any_spec = pl.BlockSpec(memory_space=pl.ANY)
        dma = pltpu.SemaphoreType.DMA
        grad_a, grad_bt, loss, _ = pl.pallas_call(
            functools.partial(kernel, stages, num_micro, ring),
            out_shape=(jax.ShapeDtypeStruct((2, model, hidden), F32), jax.ShapeDtypeStruct((2, model, hidden), F32), jax.ShapeDtypeStruct((8, 128), F32), jax.ShapeDtypeStruct((2, num_micro, tokens, hidden), BF16)),
            in_specs=[any_spec] * 4,
            out_specs=(any_spec,) * 4,
            scratch_shapes=[
                pltpu.VMEM((2, model, hidden), BF16),
                pltpu.VMEM((2, hidden, model), BF16),
                pltpu.VMEM((2, hidden, model), BF16),
                pltpu.VMEM((2, model, hidden), BF16),
                pltpu.VMEM((2, num_micro, tokens, model), BF16),
                pltpu.VMEM((2, num_micro, tokens, hidden), BF16),
                pltpu.VMEM((2, num_micro, tokens, model), BF16),
                pltpu.VMEM((2, ring, tokens, hidden), BF16),
                pltpu.VMEM((2, GROUP, tokens, hidden), BF16),
                pltpu.VMEM((2, 2, model, hidden), F32),
                pltpu.VMEM((2, tokens, hidden), BF16),
                pltpu.VMEM((2, tokens, hidden), BF16),
                pltpu.VMEM((tokens, model), BF16),
                pltpu.VMEM((tokens, model), BF16),
                pltpu.VMEM((SENDS, tokens, model), BF16),
                pltpu.VMEM((model, GROUP * tokens), BF16),
                pltpu.VMEM((8, 128), F32),
                dma((num_micro * HALVES,)), dma((num_micro * HALVES,)), dma((num_micro * HALVES,)), dma((SENDS * HALVES,)),
                dma((2,)), dma(()), dma(()), dma((2, 2)), dma((ring,)), dma((2,)),
            ],
            compiler_params=pltpu.CompilerParams(collective_id=0, has_side_effects=True, vmem_limit_bytes=67043328),
        )(micro_in, targets, w_in[0], w_out[0])
        grad_a, grad_b, total = write_results(grad_a, grad_bt, loss)
        return grad_a[None], grad_b[None], total

    return jax.shard_map(per_device, mesh=mesh, in_specs=(P('data'), P('data'), P('stage'), P('stage')), out_specs=(P(('data', 'stage')), P(('data', 'stage')), P('data')), check_vma=False)
```
